16 devices in a mesh: dp: 2 (over y, z), tp: 8 (over x, core).
Axes of the slice: x: 4, y: 2, z: 1, core: 2. Of those that a mesh axis runs over, the one named last changes fastest.
The devices are a block of a 4x4x8 slice.
Arguments:
- x: bfloat16 [8, 512, 5120], P('dp'), parts along dimension 0
- gain_a: bfloat16 [5120], replicated
- wq: bfloat16 [5120, 5120], P(None, 'tp')
- wk: bfloat16 [5120, 1024], P(None, 'tp')
- wv: bfloat16 [5120, 1024], P(None, 'tp')
- wo: bfloat16 [5120, 5120], P('tp')
- gain_m: bfloat16 [5120], replicated
- w_gate: bfloat16 [5120, 17408], P(None, 'tp')
- w_up: bfloat16 [5120, 17408], P(None, 'tp')
- w_down: bfloat16 [17408, 5120], P('tp')
Outputs:
- output: bfloat16 [8, 512, 5120], P('dp'), parts along dimension 0
There are 2 independent parts. The reference program is written for one: setup_inputs(seed, part) draws one part's arguments, and reference() takes and returns one part's arrays. A program takes and returns all parts, laid end to end along the dimension named above; an argument that names none is the same for every part.
All inputs are finite; a program needn't handle non-finite values.
Results may differ from the reference program's by a relative error of at most 0.017.
Values are sent between devices in bfloat16 or wider.
A program may use at most 768 MiB of HBM per device.

```python
import jax
import jax.numpy as jnp
from jax import lax

SEQUENCES = 4
TOKENS = 512
D = 5120
HEADS = 40
KV_HEADS = 8
HEAD = 128
FF = 17408
THETA = 10000


def setup_inputs(seed: int = 0, part: int = 0) -> dict:
    kx, ka, km, kq, kk, kv, ko, kg, ku, kd = jax.random.split(jax.random.key(seed), 10)

    def weights(key, rows, columns):
        return jax.random.normal(key, (rows, columns), jnp.float32) * rows**-0.5

    drawn = {
        "x": jax.random.normal(jax.random.fold_in(kx, part), (SEQUENCES, TOKENS, D), jnp.float32),
        "gain_a": 1 + 0.1 * jax.random.normal(ka, (D,), jnp.float32),
        "wq": 2 * weights(kq, D, HEADS * HEAD),
        "wk": 2 * weights(kk, D, KV_HEADS * HEAD),
        "wv": 4 * weights(kv, D, KV_HEADS * HEAD),
        "wo": weights(ko, HEADS * HEAD, D),
        "gain_m": 1 + 0.1 * jax.random.normal(km, (D,), jnp.float32),
        "w_gate": weights(kg, D, FF),
        "w_up": weights(ku, D, FF),
        "w_down": 3 * weights(kd, FF, D),
    }
    return {k: v.astype(jnp.bfloat16) for k, v in drawn.items()}


def normed(x, gain):
    wide = x.astype(jnp.float32)
    scale = lax.rsqrt(jnp.mean(wide * wide, -1, keepdims=True) + 1e-6)
    return (wide * scale * gain.astype(jnp.float32)).astype(jnp.bfloat16)


def turned(t, place, theta):
    half = t.shape[-1] // 2
    angle = place.astype(jnp.float32)[:, None] * theta ** (-jnp.arange(half, dtype=jnp.float32) / half)
    cos, sin = jnp.cos(angle)[:, None], jnp.sin(angle)[:, None]
    a, b = t[..., :half].astype(jnp.float32), t[..., half:].astype(jnp.float32)
    return jnp.concatenate([a * cos - b * sin, b * cos + a * sin], -1).astype(jnp.bfloat16)


def matmul(a, w):
    return jnp.dot(a, w, preferred_element_type=jnp.float32).astype(jnp.bfloat16)


def einsum(form, a, b):
    return jnp.einsum(form, a.astype(jnp.float32), b.astype(jnp.float32))


def attention(q, k, v):
    scores = einsum("tgsd,ugd->gstu", q, k) * q.shape[-1] ** -0.5
    token = jnp.arange(q.shape[0])
    scores = jnp.where(token[:, None] >= token, scores, -jnp.inf)
    weights = jax.nn.softmax(scores, -1).astype(jnp.bfloat16)
    return einsum("gstu,ugd->tgsd", weights, v).astype(jnp.bfloat16)


def one(x, gain_a, wq, wk, wv, wo, gain_m, w_gate, w_up, w_down):
    rows = x.shape[0]
    a, place = normed(x, gain_a), jnp.arange(rows)
    k = turned(matmul(a, wk).reshape(rows, -1, HEAD), place, THETA)
    q = turned(matmul(a, wq).reshape(rows, -1, HEAD), place, THETA).reshape(rows, k.shape[1], -1, HEAD)
    v = matmul(a, wv).reshape(rows, -1, HEAD)
    seen = attention(q, k, v).reshape(rows, -1)
    h = (x.astype(jnp.float32) + jnp.dot(seen, wo, preferred_element_type=jnp.float32)).astype(jnp.bfloat16)
    b = normed(h, gain_m)
    gate = jnp.dot(b, w_gate, preferred_element_type=jnp.float32)
    up = jnp.dot(b, w_up, preferred_element_type=jnp.float32)
    hidden = (jax.nn.silu(gate) * up).astype(jnp.bfloat16)
    return (h.astype(jnp.float32) + jnp.dot(hidden, w_down, preferred_element_type=jnp.float32)).astype(jnp.bfloat16)


def reference(x, gain_a, wq, wk, wv, wo, gain_m, w_gate, w_up, w_down):
    return lax.map(lambda sequence: one(sequence, gain_a, wq, wk, wv, wo, gain_m, w_gate, w_up, w_down), x)
```

```python
import functools

import jax
import jax.numpy as jnp
from jax import lax
from jax.experimental import pallas as pl
from jax.experimental.pallas import tpu as pltpu
from jax.sharding import PartitionSpec as P

HEAD = 128
THETA = 10000
TILE = 512
LANE = 128
SLOTS = 3
GROUP = 16
BF = jnp.bfloat16
F32 = jnp.float32


def layer(axis, chips, x, ga, wq, wk, wv, wo, gm, wg, wu, wd, cos, sin, y,
          wa, wt, xa, qkv, seen, hid, bb, part, sb, rr, st, mr, own, xr, hh,
          x_sem, wa_sem, wt_sem, xr_sem, y_sem, r_send, r_recv, m_send, m_recv, g_send, g_recv, d_send, d_recv, credit):
    units, rows, d = x.shape
    last = 2 * units
    half = rows // 2
    chunk = half // chips
    piece = chunk // 2
    qw, kw = wq.shape[1], wk.shape[1]
    heads = qw // HEAD
    ff = wg.shape[1]
    steps = ff // LANE
    tiles = d // TILE
    me = lax.axis_index(axis)
    core, j = lax.rem(me, 2), lax.div(me, 2)
    chip = lambda by: lax.rem(j + by + chips, chips)
    left, right, twin = chip(-1) * 2 + core, chip(1) * 2 + core, j * 2 + 1 - core
    loop = lambda n, f: lax.fori_loop(0, n, lambda i, _: (f(i), None)[1], None)

    def remote(src, dst, send, recv, to):
        return pltpu.make_async_remote_copy(src_ref=src, dst_ref=dst, send_sem=send, recv_sem=recv, device_id={axis: to},
                                            device_id_type=pl.DeviceIdType.MESH)

    def m_copy(k, par):
        return remote(st.at[k], mr.at[par, k], m_send.at[k], m_recv.at[par, k], left if k % 2 else right)

    def at(by, low, n=piece):
        return pl.ds(pl.multiple_of(chip(by) * chunk + low * piece, piece), n)

    sent = ((0, 0), (0, 1), (0, 1), (0, 0), (-1, 0), (1, 1))
    came = ((-1, 0), (1, 1), (-1, 1), (1, 0), (2, 0), (2, 1))

    def g_copy(k, par, where=sent):
        ref = bb.at[par, 0, at(*where[k])]
        return remote(ref, ref, g_send.at[par, k], g_recv.at[par, k], left if k % 2 else right)

    handed = ((0, 0, chunk), (-1, 0), (1, 1), (-1, 1), (1, 0), (2, 0, chunk))

    def d_copy(k, par):
        here = at(*handed[k])
        return remote(bb.at[par, 0, here], bb.at[par, 1, here], d_send.at[par, k], d_recv.at[par, k], twin)

    def r_copy(n, par):
        cols = pl.ds(pl.multiple_of(n * TILE, TILE), TILE)
        return remote(sb.at[:, cols], rr.at[par, :, cols], r_send.at[n], r_recv.at[par, n], twin)

    def y_copy(k, v):
        par = lax.rem(v, 2)
        where = pl.ds(pl.multiple_of((core if k == 0 else 1 - core) * half, half), half)
        return pltpu.make_async_copy(bb.at[par, k], y.at[v - units, where], y_sem.at[k])

    def x_copy(u):
        return pltpu.make_async_copy(x.at[u], xa, x_sem)

    def xr_copy(u):
        where = pl.ds(pl.multiple_of(core * half + j * chunk, chunk), chunk)
        return pltpu.make_async_copy(x.at[u, where], xr, xr_sem)

    first_weights = [pltpu.make_async_copy(w, wa.at[:, a : a + w.shape[1]], wa_sem.at[n, 0])
                     for n, (w, a) in enumerate(((wq, 0), (wk, qw), (wv, qw + kw)))]

    def gu_copies(g):
        n, slot = lax.rem(g, steps), lax.rem(g, SLOTS)
        cols = pl.ds(pl.multiple_of(n * LANE, LANE), LANE)
        return [pltpu.make_async_copy(w.at[:, cols], wa.at[:, pl.ds(pl.multiple_of(slot * 2 * LANE + k * LANE, LANE), LANE)], wa_sem.at[slot, k])
                for k, w in enumerate((wg, wu))]

    def tile_copy(w, n):
        cols = pl.ds(pl.multiple_of(n * TILE, TILE), TILE)
        slot = lax.rem(n, 2)
        return pltpu.make_async_copy(w.at[:, cols], wt.at[: w.shape[0], pl.ds(pl.multiple_of(slot * TILE, TILE), TILE)], wt_sem.at[slot])

    def unit_norm(wide, gain):
        scale = lax.rsqrt(jnp.mean(wide * wide, -1, keepdims=True) + 1e-6)
        return (wide * scale * gain[...].astype(F32)).astype(BF)

    def attend(u):
        x_copy(u).wait()

        def norm_rows(i):
            here = pl.ds(pl.multiple_of(i * GROUP, GROUP), GROUP)
            xa[here, :] = unit_norm(xa[here, :].astype(F32), ga)

        loop(rows // GROUP, norm_rows)

        @pl.when(u == 0)
        def _():
            for c in first_weights:
                c.wait()

        def project(i):
            here = pl.ds(pl.multiple_of(i * half, half), half)
            got = jnp.dot(xa[here, :], wa[...], preferred_element_type=F32).astype(BF)
            c, s = cos[here, :], sin[here, :]
            for n in range(heads + 2):
                t = got[:, n * HEAD : (n + 1) * HEAD]
                if n < heads + 1:
                    w = t.astype(F32)
                    t = (w * c + pltpu.roll(w, HEAD // 2, 1) * s).astype(BF)
                qkv[here, n * HEAD : (n + 1) * HEAD] = t

        loop(2, project)

        @pl.when(u + 1 < units)
        def _():
            x_copy(u + 1).start()

        def head(n):
            cols = pl.ds(pl.multiple_of(n * HEAD, HEAD), HEAD)
            for i in range(2):
                keys = (i + 1) * half
                q, k, v = qkv[i * half : keys, cols], qkv[:keys, qw : qw + HEAD], qkv[:keys, qw + kw : qw + kw + HEAD]
                s = lax.dot_general(q, k, (((1,), (1,)), ((), ())), preferred_element_type=F32) * HEAD**-0.5
                ok = lax.broadcasted_iota(jnp.int32, s.shape, 0) + i * half >= lax.broadcasted_iota(jnp.int32, s.shape, 1)
                s = jnp.where(ok, s, -jnp.inf)
                e = jnp.exp(s - jnp.max(s, -1, keepdims=True))
                w = (e / jnp.sum(e, -1, keepdims=True)).astype(BF)
                to = pl.ds(pl.multiple_of((core if i == 0 else 1 - core) * half, half), half)
                seen[lax.rem(u, 2), to, cols] = jnp.dot(w, v, preferred_element_type=F32).astype(BF)

        loop(heads, head)

    def gate_up(u, lo, hi):
        par = lax.rem(u, 2)

        def one(i):
            n = lo + i
            g = u * steps + n

            @pl.when(g + SLOTS - 1 < units * steps)
            def _():
                for c in gu_copies(g + SLOTS - 1):
                    c.start()

            for c in gu_copies(g):
                c.wait()
            w = wa[:, pl.ds(pl.multiple_of(lax.rem(g, SLOTS) * 2 * LANE, 2 * LANE), 2 * LANE)]
            got = jnp.dot(bb[par].reshape(rows, d), w, preferred_element_type=F32)
            gate, up = got[:, :LANE], got[:, LANE:]
            hid[par, :, pl.ds(pl.multiple_of(n * LANE, LANE), LANE)] = (gate / (1 + jnp.exp(-gate)) * up).astype(BF)

        loop(hi - lo, one)

    def outward(t, src, w):
        par = lax.rem(t + 1, 2)

        def one(n):
            @pl.when(n + 1 < tiles)
            def _():
                tile_copy(w, n + 1).start()

            tile_copy(w, n).wait()
            got = jnp.dot(src(), wt[: w.shape[0], pl.ds(pl.multiple_of(lax.rem(n, 2) * TILE, TILE), TILE)], preferred_element_type=F32)
            cols = pl.ds(pl.multiple_of(n * TILE, TILE), TILE)
            sb[:, cols] = got[half:].astype(BF)
            part[:, cols] = got[:half]
            r_copy(n, par).start()

        loop(tiles, one)

        @pl.when(t < units - 2)
        def _():
            tile_copy(wo, 0).start()

        @pl.when((t >= units - 2) & (t < last - 2))
        def _():
            tile_copy(wd, 0).start()

    def stage(k, par, by, low, extra=None):
        def some(i):
            here = pl.ds(pl.multiple_of(chip(by) * chunk + low * piece + i * GROUP, GROUP), GROUP)
            into = pl.ds(pl.multiple_of(i * GROUP, GROUP), GROUP)
            v = part[here, :] + rr[par, here, :].astype(F32)
            if extra is not None:
                v = v + mr[par, extra, into, :].astype(F32)
            st[k, into, :] = v.astype(BF)

        loop(piece // GROUP, some)
        m_copy(k, par).start()

    def p1(t):
        par = lax.rem(t, 2)

        @pl.when((t >= 1) & (t <= last))
        def _():
            for k in range(4):
                m_copy(k, par).wait_send()

        @pl.when((t >= 0) & (t < last))
        def _():
            def arrived(n):
                r_copy(n, par).wait_recv()
                r_copy(n, par).wait_send()

            loop(tiles, arrived)
            stage(0, par, 2, 0)
            stage(1, par, 2, 1)
            stage(2, par, 1, 1)
            stage(3, par, -1, 0)

        @pl.when((t >= 2) & (t < last + 2))
        def _():
            for k in (2, 3):
                g_copy(k, par, came).wait_recv()
            for k in (3, 4):
                d_copy(k, par).start()
            for k in (4, 5):
                g_copy(k, par, came).wait_recv()
            d_copy(5, par).start()
            for k in range(6):
                d_copy(k, par).wait_recv()

        @pl.when((t >= 2 + units) & (t < last + 2))
        def _():
            for k in range(2):
                y_copy(k, t - 2).start()

    def p2(t):
        v = t - 1
        par = lax.rem(v, 2)

        @pl.when((t >= 1) & (t <= last))
        def _():
            for k in (2, 3, 4, 5):
                m_copy(k, par).wait_recv()

            def finish(residual, store):
                for low, ks in enumerate(((4, 3), (2, 5))):
                    def some(i):
                        inner = pl.ds(pl.multiple_of(i * GROUP, GROUP), GROUP)
                        here = pl.ds(pl.multiple_of(low * piece + i * GROUP, GROUP), GROUP)
                        s = own[here, :] + mr[par, ks[0], inner, :].astype(F32) + mr[par, ks[1], inner, :].astype(F32)
                        s = (residual(here).astype(F32) + s).astype(BF)
                        bb[par, 0, pl.ds(pl.multiple_of(j * chunk + low * piece + i * GROUP, GROUP), GROUP), :] = store(here, s)

                    loop(piece // GROUP, some)

            @pl.when(v < units)
            def _():
                xr_copy(v).wait()

                def store(here, s):
                    hh[v, here, :] = s
                    return unit_norm(s.astype(F32), gm)

                finish(lambda here: xr[here, :], store)

            @pl.when(v >= units)
            def _():
                finish(lambda here: hh[v - units, here, :], lambda here, s: s)

            for k in range(4):
                g_copy(k, par).start()

        @pl.when((t >= 3) & (t <= last))
        def _():
            pl.semaphore_wait(credit, 1)

        @pl.when((t >= 1) & (t <= last))
        def _():
            d_copy(0, par).start()

    def p3(t):
        par, old = lax.rem(t, 2), lax.rem(t + 1, 2)

        @pl.when((t >= 2 + units) & (t < last + 2))
        def _():
            for k in range(2):
                y_copy(k, t - 2).wait()

        @pl.when((t >= 2) & (t < last + 2))
        def _():
            for k in range(6):
                g_copy(k, par).wait_send()
                d_copy(k, par).wait_send()

        @pl.when((t >= 2) & (t < last))
        def _():
            pl.semaphore_signal(credit, inc=1, device_id={axis: twin}, device_id_type=pl.DeviceIdType.MESH)

        @pl.when((t >= 1) & (t <= last))
        def _():
            for k in (4, 5):
                m_copy(k, par).wait_send()

        @pl.when((t >= 0) & (t < last))
        def _():
            m_copy(0, par).wait_recv()
            stage(4, par, 1, 0, 0)
            m_copy(1, par).wait_recv()
            stage(5, par, -1, 1, 1)

            def keep(i):
                here = pl.ds(pl.multiple_of(j * chunk + i * GROUP, GROUP), GROUP)
                own[pl.ds(pl.multiple_of(i * GROUP, GROUP), GROUP), :] = part[here, :] + rr[par, here, :].astype(F32)

            loop(chunk // GROUP, keep)

        @pl.when((t >= 0) & (t < units))
        def _():
            xr_copy(t).start()

        @pl.when((t >= 1) & (t <= last))
        def _():
            for k in range(2):
                g_copy(k, old, came).wait_recv()
                g_copy(4 + k, old).start()
            for k in range(2):
                d_copy(1 + k, old).start()

    x_copy(0).start()
    for c in first_weights:
        c.start()
    tile_copy(wo, 0).start()
    barrier = pltpu.get_barrier_semaphore()
    for peer in (left, right, twin):
        pl.semaphore_signal(barrier, inc=1, device_id={axis: peer}, device_id_type=pl.DeviceIdType.MESH)
    pl.semaphore_wait(barrier, 3)

    cut = steps // 2

    def period(i):
        t = i - 1
        busy = (t >= 2) & (t < units + 2)
        p1(t)

        @pl.when(t < units - 2)
        def _():
            attend(t + 1)

        @pl.when(busy)
        def _():
            gate_up(t - 2, 0, cut)

        p2(t)

        @pl.when(t == units - 3)
        def _():
            attend(t + 2)
            for g in range(SLOTS - 1):
                for c in gu_copies(jnp.int32(g)):
                    c.start()

        @pl.when(busy)
        def _():
            gate_up(t - 2, cut, steps)

        p3(t)

        @pl.when(t < units - 1)
        def _():
            outward(t, lambda: seen[lax.rem(t + 1, 2)], wo)

        @pl.when((t >= units - 1) & (t < last - 1))
        def _():
            par = lax.rem(t - units + 1, 2)
            outward(t, lambda: hid[par], wd)

    loop(last + 3, period)


def solution(mesh):
    axis = "tp"
    chips = mesh.shape[axis] // 2

    def step(x, gain_a, wq, wk, wv, wo, gain_m, w_gate, w_up, w_down):
        units, rows, d = x.shape
        half, ff = rows // 2, w_gate.shape[1]
        chunk = half // chips
        qkv_width = wq.shape[1] + wk.shape[1] + wv.shape[1]
        place = jnp.arange(rows)
        angle = place.astype(F32)[:, None] * THETA ** (-jnp.arange(HEAD // 2, dtype=F32) / (HEAD // 2))
        cos, sin = jnp.cos(angle), jnp.sin(angle)
        cos, sin = jnp.concatenate([cos, cos], 1), jnp.concatenate([-sin, sin], 1)
        hbm, vmem = pl.BlockSpec(memory_space=pl.ANY), pl.BlockSpec(memory_space=pltpu.VMEM)
        dma = lambda *shape: pltpu.SemaphoreType.DMA(shape)
        tiles = d // TILE
        return pl.pallas_call(
            functools.partial(layer, axis, chips),
            out_shape=jax.ShapeDtypeStruct(x.shape, x.dtype),
            in_specs=[hbm, vmem, hbm, hbm, hbm, hbm, vmem, hbm, hbm, hbm, vmem, vmem],
            out_specs=hbm,
            scratch_shapes=[
                pltpu.VMEM((d, qkv_width), BF),
                pltpu.VMEM((max(ff, wo.shape[0]), 2 * TILE), BF),
                pltpu.VMEM((rows, d), BF),
                pltpu.VMEM((rows, qkv_width), BF),
                pltpu.VMEM((2, rows, wq.shape[1]), BF),
                pltpu.VMEM((2, rows, ff), BF),
                pltpu.VMEM((2, 2, half, d), BF),
                pltpu.VMEM((half, d), F32),
                pltpu.VMEM((half, d), BF),
                pltpu.VMEM((2, half, d), BF),
                pltpu.VMEM((6, chunk // 2, d), BF),
                pltpu.VMEM((2, 6, chunk // 2, d), BF),
                pltpu.VMEM((chunk, d), F32),
                pltpu.VMEM((chunk, d), BF),
                pltpu.VMEM((units, chunk, d), BF),
                pltpu.SemaphoreType.DMA,
                dma(SLOTS, 2), dma(2), pltpu.SemaphoreType.DMA, dma(2),
                dma(tiles), dma(2, tiles), dma(6), dma(2, 6), dma(2, 6), dma(2, 6), dma(2, 6), dma(2, 6),
                pltpu.SemaphoreType.REGULAR,
            ],
            compiler_params=pltpu.CompilerParams(collective_id=0, has_side_effects=True, vmem_limit_bytes=67043328),
        )(x, gain_a[None], wq, wk, wv, wo, gain_m[None], w_gate, w_up, w_down, cos, sin)

    tokens, whole, columns, rows_of = P("dp", None, None), P(None), P(None, "tp"), P("tp", None)
    return jax.shard_map(
        step,
        mesh=mesh,
        in_specs=(tokens, whole, columns, columns, columns, rows_of, whole, columns, columns, rows_of),
        out_specs=tokens,
        check_vma=False,
    )
```

```python
import functools

import jax
import jax.numpy as jnp
from jax import lax
from jax.experimental import pallas as pl
from jax.experimental.pallas import tpu as pltpu
from jax.sharding import PartitionSpec as P

HEAD = 128
THETA = 10000
TILE = 512
LANE = 128
SLOTS = 3
GROUP = 16
BF = jnp.bfloat16
F32 = jnp.float32


def layer(axis, chips, x, ga, wq, wk, wv, wo, gm, wg, wu, wd, cos, sin, y,
          wa, wt, xa, qkv, seen, hid, bb, part, sb, rr, st, mr, own, xr, hh, gains,
          x_sem, wa_sem, wt_sem, xr_sem, y_sem, r_send, r_recv, m_send, m_recv, g_send, g_recv, d_send, d_recv, credit):
    units, rows, d = x.shape
    last = 2 * units
    half = rows // 2
    chunk = half // chips
    piece = chunk // 2
    qw, kw = wq.shape[1], wk.shape[1]
    heads = qw // HEAD
    ff = wg.shape[1]
    steps = ff // LANE
    tiles = d // TILE
    me = lax.axis_index(axis)
    core, j = lax.rem(me, 2), lax.div(me, 2)
    chip = lambda by: lax.rem(j + by + chips, chips)
    left, right, twin = chip(-1) * 2 + core, chip(1) * 2 + core, j * 2 + 1 - core
    loop = lambda n, f: lax.fori_loop(0, n, lambda i, _: (f(i), None)[1], None)

    def remote(src, dst, send, recv, to):
        return pltpu.make_async_remote_copy(src_ref=src, dst_ref=dst, send_sem=send, recv_sem=recv, device_id={axis: to},
                                            device_id_type=pl.DeviceIdType.MESH)

    def m_copy(k, par):
        return remote(st.at[k], mr.at[par, k], m_send.at[k], m_recv.at[par, k], left if k % 2 else right)

    def at(by, low, n=piece):
        return pl.ds(pl.multiple_of(chip(by) * chunk + low * piece, piece), n)

    sent = ((0, 0), (0, 1), (0, 1), (0, 0), (-1, 0), (1, 1))
    came = ((-1, 0), (1, 1), (-1, 1), (1, 0), (2, 0), (2, 1))

    def g_copy(k, par, where=sent):
        ref = bb.at[par, 0, at(*where[k])]
        return remote(ref, ref, g_send.at[par, k], g_recv.at[par, k], left if k % 2 else right)

    handed = ((0, 0, chunk), (-1, 0), (1, 1), (-1, 1), (1, 0), (2, 0, chunk))

    def d_copy(k, par):
        here = at(*handed[k])
        return remote(bb.at[par, 0, here], bb.at[par, 1, here], d_send.at[par, k], d_recv.at[par, k], twin)

    def r_copy(n, par):
        cols = pl.ds(pl.multiple_of(n * TILE, TILE), TILE)
        return remote(sb.at[:, cols], rr.at[par, :, cols], r_send.at[n], r_recv.at[par, n], twin)

    def y_copy(k, v):
        par = lax.rem(v, 2)
        where = pl.ds(pl.multiple_of((core if k == 0 else 1 - core) * half, half), half)
        return pltpu.make_async_copy(bb.at[par, k], y.at[v - units, where], y_sem.at[k])

    def x_copy(u):
        return pltpu.make_async_copy(x.at[u], xa, x_sem)

    def xr_copy(u):
        where = pl.ds(pl.multiple_of(core * half + j * chunk, chunk), chunk)
        return pltpu.make_async_copy(x.at[u, where], xr, xr_sem)

    first_weights = [pltpu.make_async_copy(w, wa.at[:, a : a + w.shape[1]], wa_sem.at[n, 0])
                     for n, (w, a) in enumerate(((wq, 0), (wk, qw), (wv, qw + kw)))]

    def gu_copies(g):
        n, slot = lax.rem(g, steps), lax.rem(g, SLOTS)
        cols = pl.ds(pl.multiple_of(n * LANE, LANE), LANE)
        return [pltpu.make_async_copy(w.at[:, cols], wa.at[:, pl.ds(pl.multiple_of(slot * 2 * LANE + k * LANE, LANE), LANE)], wa_sem.at[slot, k])
                for k, w in enumerate((wg, wu))]

    def tile_copy(w, n):
        cols = pl.ds(pl.multiple_of(n * TILE, TILE), TILE)
        slot = lax.rem(n, 2)
        return pltpu.make_async_copy(w.at[:, cols], wt.at[: w.shape[0], pl.ds(pl.multiple_of(slot * TILE, TILE), TILE)], wt_sem.at[slot])

    def unit_norm(wide, which):
        scale = lax.rsqrt(jnp.mean(wide * wide, -1, keepdims=True) + 1e-6)
        return (wide * scale * gains[which : which + 1, :]).astype(BF)

    def attend(u):
        x_copy(u).wait()

        def norm_rows(i):
            here = pl.ds(pl.multiple_of(i * GROUP, GROUP), GROUP)
            xa[here, :] = unit_norm(xa[here, :].astype(F32), 0)

        loop(rows // GROUP, norm_rows)

        @pl.when(u == 0)
        def _():
            for c in first_weights:
                c.wait()

        def project(i):
            here = pl.ds(pl.multiple_of(i * half, half), half)
            got = jnp.dot(xa[here, :], wa[...], preferred_element_type=F32).astype(BF)
            c, s = cos[here, :], sin[here, :]
            for n in range(heads + 2):
                t = got[:, n * HEAD : (n + 1) * HEAD]
                if n < heads + 1:
                    w = t.astype(F32)
                    t = (w * c + pltpu.roll(w, HEAD // 2, 1) * s).astype(BF)
                qkv[here, n * HEAD : (n + 1) * HEAD] = t

        loop(2, project)

        @pl.when(u + 1 < units)
        def _():
            x_copy(u + 1).start()

        def head(n):
            cols = pl.ds(pl.multiple_of(n * HEAD, HEAD), HEAD)
            for i in range(2):
                keys = (i + 1) * half
                q, k, v = qkv[i * half : keys, cols], qkv[:keys, qw : qw + HEAD], qkv[:keys, qw + kw : qw + kw + HEAD]
                s = lax.dot_general(q, k, (((1,), (1,)), ((), ())), preferred_element_type=F32) * HEAD**-0.5
                ok = lax.broadcasted_iota(jnp.int32, s.shape, 0) + i * half >= lax.broadcasted_iota(jnp.int32, s.shape, 1)
                s = jnp.where(ok, s, -jnp.inf)
                e = jnp.exp(s - jnp.max(s, -1, keepdims=True))
                w = (e / jnp.sum(e, -1, keepdims=True)).astype(BF)
                to = pl.ds(pl.multiple_of((core if i == 0 else 1 - core) * half, half), half)
                seen[lax.rem(u, 2), to, cols] = jnp.dot(w, v, preferred_element_type=F32).astype(BF)

        loop(heads, head)

    def gate_up(u, lo, hi):
        par = lax.rem(u, 2)

        def one(i):
            n = lo + i
            g = u * steps + n

            @pl.when(g + SLOTS - 1 < units * steps)
            def _():
                for c in gu_copies(g + SLOTS - 1):
                    c.start()

            for c in gu_copies(g):
                c.wait()
            w = wa[:, pl.ds(pl.multiple_of(lax.rem(g, SLOTS) * 2 * LANE, 2 * LANE), 2 * LANE)]
            got = jnp.dot(bb[par].reshape(rows, d), w, preferred_element_type=F32)
            gate, up = got[:, :LANE], got[:, LANE:]
            hid[par, :, pl.ds(pl.multiple_of(n * LANE, LANE), LANE)] = (gate / (1 + jnp.exp(-gate)) * up).astype(BF)

        loop(hi - lo, one)

    def outward(t, src, w):
        par = lax.rem(t + 1, 2)

        def one(n):
            @pl.when(n + 1 < tiles)
            def _():
                tile_copy(w, n + 1).start()

            tile_copy(w, n).wait()
            got = jnp.dot(src(), wt[: w.shape[0], pl.ds(pl.multiple_of(lax.rem(n, 2) * TILE, TILE), TILE)], preferred_element_type=F32)
            cols = pl.ds(pl.multiple_of(n * TILE, TILE), TILE)
            sb[:, cols] = got[half:].astype(BF)
            part[:, cols] = got[:half]
            r_copy(n, par).start()

        loop(tiles, one)

        @pl.when(t < units - 2)
        def _():
            tile_copy(wo, 0).start()

        @pl.when((t >= units - 2) & (t < last - 2))
        def _():
            tile_copy(wd, 0).start()

    def stage(k, par, by, low, extra=None):
        def some(i):
            here = pl.ds(pl.multiple_of(chip(by) * chunk + low * piece + i * GROUP, GROUP), GROUP)
            into = pl.ds(pl.multiple_of(i * GROUP, GROUP), GROUP)
            v = part[here, :] + rr[par, here, :].astype(F32)
            if extra is not None:
                v = v + mr[par, extra, into, :].astype(F32)
            st[k, into, :] = v.astype(BF)

        loop(piece // GROUP, some)
        m_copy(k, par).start()

    def p1(t):
        par = lax.rem(t, 2)

        @pl.when((t >= 1) & (t <= last))
        def _():
            for k in range(4):
                m_copy(k, par).wait_send()

        @pl.when((t >= 0) & (t < last))
        def _():
            def arrived(n):
                r_copy(n, par).wait_recv()
                r_copy(n, par).wait_send()

            loop(tiles, arrived)
            stage(0, par, 2, 0)
            stage(1, par, 2, 1)
            stage(2, par, 1, 1)
            stage(3, par, -1, 0)

    def p2(t):
        v = t - 1
        par, old = lax.rem(t + 1, 2), lax.rem(t, 2)

        @pl.when((t >= 3) & (t <= last))
        def _():
            for k, peer in enumerate((right, left, twin)):
                pl.semaphore_signal(credit.at[k], inc=1, device_id={axis: peer}, device_id_type=pl.DeviceIdType.MESH)

        @pl.when((t >= 1) & (t <= last))
        def _():
            for k in (2, 3, 4, 5):
                m_copy(k, par).wait_recv()

            def finish(residual, store):
                for low, ks in enumerate(((4, 3), (2, 5))):
                    def some(i):
                        inner = pl.ds(pl.multiple_of(i * GROUP, GROUP), GROUP)
                        here = pl.ds(pl.multiple_of(low * piece + i * GROUP, GROUP), GROUP)
                        s = own[here, :] + mr[par, ks[0], inner, :].astype(F32) + mr[par, ks[1], inner, :].astype(F32)
                        s = (residual(here).astype(F32) + s).astype(BF)
                        bb[par, 0, pl.ds(pl.multiple_of(j * chunk + low * piece + i * GROUP, GROUP), GROUP), :] = store(here, s)

                    loop(piece // GROUP, some)

            @pl.when(v < units)
            def _():
                xr_copy(v).wait()

                def store(here, s):
                    hh[v, here, :] = s
                    return unit_norm(s.astype(F32), 1)

                finish(lambda here: xr[here, :], store)

            @pl.when(v >= units)
            def _():
                finish(lambda here: hh[v - units, here, :], lambda here, s: s)

            @pl.when(t >= 3)
            def _():
                for k in range(3):
                    pl.semaphore_wait(credit.at[k], 1)

            for k in range(4):
                g_copy(k, par).start()
            d_copy(0, par).start()

        @pl.when((t >= 2) & (t < last + 2))
        def _():
            for k in (2, 3):
                g_copy(k, old, came).wait_recv()
            for k in (3, 4):
                d_copy(k, old).start()
            for k in (4, 5):
                g_copy(k, old, came).wait_recv()
            d_copy(5, old).start()
            for k in range(6):
                d_copy(k, old).wait_recv()

        @pl.when((t >= 2 + units) & (t < last + 2))
        def _():
            for k in range(2):
                y_copy(k, t - 2).start()

    def p3(t):
        par, old = lax.rem(t, 2), lax.rem(t + 1, 2)

        @pl.when((t >= 2 + units) & (t < last + 2))
        def _():
            for k in range(2):
                y_copy(k, t - 2).wait()

        @pl.when((t >= 2) & (t < last + 2))
        def _():
            for k in range(6):
                g_copy(k, par).wait_send()
                d_copy(k, par).wait_send()

        @pl.when((t >= 1) & (t <= last))
        def _():
            for k in (4, 5):
                m_copy(k, par).wait_send()

        @pl.when((t >= 0) & (t < last))
        def _():
            m_copy(0, par).wait_recv()
            stage(4, par, 1, 0, 0)
            m_copy(1, par).wait_recv()
            stage(5, par, -1, 1, 1)

            def keep(i):
                here = pl.ds(pl.multiple_of(j * chunk + i * GROUP, GROUP), GROUP)
                own[pl.ds(pl.multiple_of(i * GROUP, GROUP), GROUP), :] = part[here, :] + rr[par, here, :].astype(F32)

            loop(chunk // GROUP, keep)

        @pl.when((t >= 0) & (t < units))
        def _():
            xr_copy(t).start()

        @pl.when((t >= 1) & (t <= last))
        def _():
            for k in range(2):
                g_copy(k, old, came).wait_recv()
                g_copy(4 + k, old).start()
            for k in range(2):
                d_copy(1 + k, old).start()

    x_copy(0).start()
    for c in first_weights:
        c.start()
    tile_copy(wo, 0).start()
    for which, g in enumerate((ga, gm)):
        for n in range(d // LANE):
            gains[which : which + 1, n * LANE : (n + 1) * LANE] = g[n : n + 1, :].astype(F32)
    barrier = pltpu.get_barrier_semaphore()
    for peer in (left, right, twin):
        pl.semaphore_signal(barrier, inc=1, device_id={axis: peer}, device_id_type=pl.DeviceIdType.MESH)
    pl.semaphore_wait(barrier, 3)

    cut = (steps + 1) // 2

    def period(i):
        t = i - 1
        p1(t)

        @pl.when(t < units - 2)
        def _():
            attend(t + 1)

        @pl.when((t >= 3) & (t < units + 3))
        def _():
            gate_up(t - 3, cut, steps)

        p2(t)

        @pl.when(t == units - 3)
        def _():
            attend(t + 2)
            for g in range(SLOTS - 1):
                for c in gu_copies(jnp.int32(g)):
                    c.start()

        @pl.when((t >= 2) & (t < units + 2))
        def _():
            gate_up(t - 2, 0, cut)

        p3(t)

        @pl.when(t < units - 1)
        def _():
            outward(t, lambda: seen[lax.rem(t + 1, 2)], wo)

        @pl.when((t >= units - 1) & (t < last - 1))
        def _():
            par = lax.rem(t - units + 1, 2)
            outward(t, lambda: hid[par], wd)

    loop(last + 3, period)


def put_out(y, out, held, came, gone):
    per, n = held.shape[1], held.shape[0]
    rows = lambda ref, i: ref.at[i * per // ref.shape[1], pl.ds(i * per % ref.shape[1], per)]
    reads = [pltpu.make_async_copy(rows(y, i), held.at[i], came.at[i]) for i in range(n)]
    writes = [pltpu.make_async_copy(held.at[i], rows(out, i), gone.at[i]) for i in range(n)]
    for c in reads:
        c.start()
    for r, w in zip(reads, writes):
        r.wait()
        w.start()
    for w in writes:
        w.wait()


def solution(mesh):
    axis = "tp"
    chips = mesh.shape[axis] // 2

    def step(x, gain_a, wq, wk, wv, wo, gain_m, w_gate, w_up, w_down):
        units, rows, d = x.shape
        half, ff = rows // 2, w_gate.shape[1]
        chunk = half // chips
        qkv_width = wq.shape[1] + wk.shape[1] + wv.shape[1]
        place = jnp.arange(rows)
        lane = jnp.arange(HEAD)
        angle = place.astype(F32)[:, None] * THETA ** (-(lane % (HEAD // 2)).astype(F32) / (HEAD // 2))
        cos, sin = jnp.cos(angle), jnp.where(lane < HEAD // 2, -1.0, 1.0) * jnp.sin(angle)
        hbm, vmem = pl.BlockSpec(memory_space=pl.ANY), pl.BlockSpec(memory_space=pltpu.VMEM)
        dma = lambda *shape: pltpu.SemaphoreType.DMA(shape)
        tiles = d // TILE
        y = pl.pallas_call(
            functools.partial(layer, axis, chips),
            out_shape=jax.ShapeDtypeStruct(x.shape, x.dtype),
            in_specs=[hbm, vmem, hbm, hbm, hbm, hbm, vmem, hbm, hbm, hbm, vmem, vmem],
            out_specs=hbm,
            scratch_shapes=[
                pltpu.VMEM((d, qkv_width), BF),
                pltpu.VMEM((max(ff, wo.shape[0]), 2 * TILE), BF),
                pltpu.VMEM((rows, d), BF),
                pltpu.VMEM((rows, qkv_width), BF),
                pltpu.VMEM((2, rows, wq.shape[1]), BF),
                pltpu.VMEM((2, rows, ff), BF),
                pltpu.VMEM((2, 2, half, d), BF),
                pltpu.VMEM((half, d), F32),
                pltpu.VMEM((half, d), BF),
                pltpu.VMEM((2, half, d), BF),
                pltpu.VMEM((6, chunk // 2, d), BF),
                pltpu.VMEM((2, 6, chunk // 2, d), BF),
                pltpu.VMEM((chunk, d), F32),
                pltpu.VMEM((chunk, d), BF),
                pltpu.VMEM((units, chunk, d), BF),
                pltpu.VMEM((2, d), F32),
                pltpu.SemaphoreType.DMA,
                dma(SLOTS, 2), dma(2), pltpu.SemaphoreType.DMA, dma(2),
                dma(tiles), dma(2, tiles), dma(6), dma(2, 6), dma(2, 6), dma(2, 6), dma(2, 6), dma(2, 6),
                pltpu.SemaphoreType.REGULAR((3,)),
            ],
            compiler_params=pltpu.CompilerParams(collective_id=0, has_side_effects=True, vmem_limit_bytes=67043328),
        )(x, gain_a.reshape(-1, LANE), wq, wk, wv, wo, gain_m.reshape(-1, LANE), w_gate, w_up, w_down, cos, sin)
        pieces, per = units * rows // 128, 128
        return pl.pallas_call(
            put_out,
            out_shape=jax.ShapeDtypeStruct(x.shape, x.dtype),
            in_specs=[hbm],
            out_specs=hbm,
            scratch_shapes=[pltpu.VMEM((pieces, per, d), BF), dma(pieces), dma(pieces)],
            compiler_params=pltpu.CompilerParams(vmem_limit_bytes=67043328),
        )(y)

    tokens, whole, columns, rows_of = P("dp", None, None), P(None), P(None, "tp"), P("tp", None)
    return jax.shard_map(
        step,
        mesh=mesh,
        in_specs=(tokens, whole, columns, columns, columns, rows_of, whole, columns, columns, rows_of),
        out_specs=tokens,
        check_vma=False,
    )
```

```python
import functools

import jax
import jax.numpy as jnp
from jax import lax
from jax.experimental import pallas as pl
from jax.experimental.pallas import tpu as pltpu
from jax.sharding import PartitionSpec as P

HEAD = 128
THETA = 10000
TILE = 512
LANE = 128
WIDE = 256
GROUP = 16
BF = jnp.bfloat16
F32 = jnp.float32


def layer(axis, chips, x, ga, wq, wk, wv, wo, gm, wg, wu, wd, cos, sin, y,
          wa, wt, xa, qkv, seen, hid, bb, part, sb, rr, st, mr, own, xr, hh, gains,
          x_sem, wa_sem, wt_sem, xr_sem, y_sem, r_send, r_recv, m_send, m_recv, g_send, g_recv, d_send, d_recv, credit):
    units, rows, d = x.shape
    last = 2 * units
    half = rows // 2
    chunk = half // chips
    piece = chunk // 2
    qw, kw = wq.shape[1], wk.shape[1]
    heads = qw // HEAD
    ff = wg.shape[1]
    full, rest = ff // WIDE, ff % WIDE
    blocks = full + (rest > 0)
    tiles = d // TILE
    me = lax.axis_index(axis)
    core, j = lax.rem(me, 2), lax.div(me, 2)
    chip = lambda by: lax.rem(j + by + chips, chips)
    left, right, twin = chip(-1) * 2 + core, chip(1) * 2 + core, j * 2 + 1 - core
    loop = lambda n, f: lax.fori_loop(0, n, lambda i, _: (f(i), None)[1], None)

    def remote(src, dst, send, recv, to):
        return pltpu.make_async_remote_copy(src_ref=src, dst_ref=dst, send_sem=send, recv_sem=recv, device_id={axis: to},
                                            device_id_type=pl.DeviceIdType.MESH)

    def m_copy(k, par):
        return remote(st.at[k], mr.at[par, k], m_send.at[k], m_recv.at[par, k], left if k % 2 else right)

    def at(by, low, n=piece):
        return pl.ds(pl.multiple_of(chip(by) * chunk + low * piece, piece), n)

    sent = ((0, 0), (0, 1), (0, 1), (0, 0), (-1, 0), (1, 1))
    came = ((-1, 0), (1, 1), (-1, 1), (1, 0), (2, 0), (2, 1))

    def g_copy(k, par, where=sent):
        ref = bb.at[par, 0, at(*where[k])]
        return remote(ref, ref, g_send.at[par, k], g_recv.at[par, k], left if k % 2 else right)

    handed = ((0, 0, chunk), (-1, 0), (1, 1), (-1, 1), (1, 0), (2, 0, chunk))

    def d_copy(k, par):
        here = at(*handed[k])
        return remote(bb.at[par, 0, here], bb.at[par, 1, here], d_send.at[par, k], d_recv.at[par, k], twin)

    def r_copy(n, par):
        cols = pl.ds(pl.multiple_of(n * TILE, TILE), TILE)
        return remote(sb.at[:, cols], rr.at[par, :, cols], r_send.at[n], r_recv.at[par, n], twin)

    def y_copy(k, v):
        par = lax.rem(v, 2)
        where = pl.ds(pl.multiple_of((core if k == 0 else 1 - core) * half, half), half)
        return pltpu.make_async_copy(bb.at[par, k], y.at[v - units, where], y_sem.at[k])

    def x_copy(u):
        return pltpu.make_async_copy(x.at[u], xa, x_sem)

    def xr_copy(u):
        where = pl.ds(pl.multiple_of(core * half + j * chunk, chunk), chunk)
        return pltpu.make_async_copy(x.at[u, where], xr, xr_sem)

    first_weights = [pltpu.make_async_copy(w, wa.at[:, a : a + w.shape[1]], wa_sem.at[n, 0])
                     for n, (w, a) in enumerate(((wq, 0), (wk, qw), (wv, qw + kw)))]

    def gu_slot(u, n, k, width):
        return pl.ds(pl.multiple_of(lax.rem(u * blocks + n, 2) * 2 * WIDE + k * width, LANE), width)

    def gu_copies(u, n, width):
        cols = pl.ds(pl.multiple_of(n * WIDE, WIDE), width)
        return [pltpu.make_async_copy(w.at[:, cols], wa.at[:, gu_slot(u, n, k, width)], wa_sem.at[lax.rem(u * blocks + n, 2), k])
                for k, w in enumerate((wg, wu))]

    def gu_start(u, n, width):
        for c in gu_copies(u, n, width):
            c.start()

    def tile_copy(w, n):
        cols = pl.ds(pl.multiple_of(n * TILE, TILE), TILE)
        slot = lax.rem(n, 2)
        return pltpu.make_async_copy(w.at[:, cols], wt.at[: w.shape[0], pl.ds(pl.multiple_of(slot * TILE, TILE), TILE)], wt_sem.at[slot])

    def unit_norm(wide, which):
        scale = lax.rsqrt(jnp.mean(wide * wide, -1, keepdims=True) + 1e-6)
        return (wide * scale * gains[which : which + 1, :]).astype(BF)

    def attend(u):
        x_copy(u).wait()

        def norm_rows(i):
            here = pl.ds(pl.multiple_of(i * GROUP, GROUP), GROUP)
            xa[here, :] = unit_norm(xa[here, :].astype(F32), 0)

        loop(rows // GROUP, norm_rows)

        @pl.when(u == 0)
        def _():
            for c in first_weights:
                c.wait()

        def project(i):
            here = pl.ds(pl.multiple_of(i * half, half), half)
            got = jnp.dot(xa[here, :], wa[:, : qw + 2 * kw], preferred_element_type=F32).astype(BF)
            c, s = cos[here, :], sin[here, :]
            for n in range(heads + 2):
                t = got[:, n * HEAD : (n + 1) * HEAD]
                if n < heads + 1:
                    w = t.astype(F32)
                    t = (w * c + pltpu.roll(w, HEAD // 2, 1) * s).astype(BF)
                qkv[here, n * HEAD : (n + 1) * HEAD] = t

        loop(2, project)

        @pl.when(u + 1 < units)
        def _():
            x_copy(u + 1).start()

        def head(n):
            cols = pl.ds(pl.multiple_of(n * HEAD, HEAD), HEAD)
            for i in range(2):
                keys = (i + 1) * half
                q, k, v = qkv[i * half : keys, cols], qkv[:keys, qw : qw + HEAD], qkv[:keys, qw + kw : qw + kw + HEAD]
                s = lax.dot_general(q, k, (((1,), (1,)), ((), ())), preferred_element_type=F32) * HEAD**-0.5
                ok = lax.broadcasted_iota(jnp.int32, s.shape, 0) + i * half >= lax.broadcasted_iota(jnp.int32, s.shape, 1)
                s = jnp.where(ok, s, -jnp.inf)
                e = jnp.exp(s - jnp.max(s, -1, keepdims=True))
                w = (e / jnp.sum(e, -1, keepdims=True)).astype(BF)
                to = pl.ds(pl.multiple_of((core if i == 0 else 1 - core) * half, half), half)
                seen[lax.rem(u, 2), to, cols] = jnp.dot(w, v, preferred_element_type=F32).astype(BF)

        loop(heads, head)

    def gate_up(u, n, width):
        par = lax.rem(u, 2)
        if width == WIDE:
            @pl.when(n + 1 < full)
            def _():
                gu_start(u, n + 1, WIDE)

            if rest:
                @pl.when(n + 1 == full)
                def _():
                    gu_start(u, n + 1, rest)

        if width == rest or not rest:
            @pl.when((n + 1 == blocks) & (u + 1 < units))
            def _():
                gu_start(u + 1, 0, WIDE)

        for c in gu_copies(u, n, width):
            c.wait()
        slot = pl.ds(pl.multiple_of(lax.rem(u * blocks + n, 2) * 2 * WIDE, 2 * WIDE), 2 * width)
        got = jnp.dot(bb[par].reshape(rows, d), wa[:, slot], preferred_element_type=F32)
        gate, up = got[:, :width], got[:, width:]
        hid[par, :, pl.ds(pl.multiple_of(n * WIDE, WIDE), width)] = (gate / (1 + jnp.exp(-gate)) * up).astype(BF)

    def outward(t, src, w):
        par = lax.rem(t + 1, 2)

        def one(n):
            @pl.when(n + 1 < tiles)
            def _():
                tile_copy(w, n + 1).start()

            tile_copy(w, n).wait()
            got = jnp.dot(src(), wt[: w.shape[0], pl.ds(pl.multiple_of(lax.rem(n, 2) * TILE, TILE), TILE)], preferred_element_type=F32)
            cols = pl.ds(pl.multiple_of(n * TILE, TILE), TILE)
            sb[:, cols] = got[half:].astype(BF)
            part[:, cols] = got[:half]
            r_copy(n, par).start()

        loop(tiles, one)

        @pl.when(t < units - 2)
        def _():
            tile_copy(wo, 0).start()

        @pl.when((t >= units - 2) & (t < last - 2))
        def _():
            tile_copy(wd, 0).start()

    def stage(k, par, by, low, extra=None):
        def some(i):
            here = pl.ds(pl.multiple_of(chip(by) * chunk + low * piece + i * GROUP, GROUP), GROUP)
            into = pl.ds(pl.multiple_of(i * GROUP, GROUP), GROUP)
            v = part[here, :] + rr[par, here, :].astype(F32)
            if extra is not None:
                v = v + mr[par, extra, into, :].astype(F32)
            st[k, into, :] = v.astype(BF)

        loop(piece // GROUP, some)
        m_copy(k, par).start()

    def p1(t):
        par = lax.rem(t, 2)

        @pl.when((t >= 1) & (t <= last))
        def _():
            for k in range(4):
                m_copy(k, par).wait_send()

        @pl.when((t >= 0) & (t < last))
        def _():
            def arrived(n):
                r_copy(n, par).wait_recv()
                r_copy(n, par).wait_send()

            loop(tiles, arrived)
            stage(0, par, 2, 0)
            stage(1, par, 2, 1)
            stage(2, par, 1, 1)
            stage(3, par, -1, 0)

    def p2(t):
        v = t - 1
        par, old = lax.rem(t + 1, 2), lax.rem(t, 2)

        def hand_on():
            for k in (2, 3):
                g_copy(k, old, came).wait_recv()
            for k in (3, 4):
                d_copy(k, old).start()
            for k in (4, 5):
                g_copy(k, old, came).wait_recv()
            d_copy(5, old).start()

        @pl.when((t >= 3) & (t <= last))
        def _():
            for k, peer in enumerate((right, left, twin)):
                pl.semaphore_signal(credit.at[k], inc=1, device_id={axis: peer}, device_id_type=pl.DeviceIdType.MESH)

        @pl.when((t >= 2) & (t < last))
        def _():
            hand_on()

        @pl.when((t >= 1) & (t <= last))
        def _():
            for k in (2, 3, 4, 5):
                m_copy(k, par).wait_recv()

            def finish(residual, store):
                for low, ks in enumerate(((4, 3), (2, 5))):
                    def some(i):
                        inner = pl.ds(pl.multiple_of(i * GROUP, GROUP), GROUP)
                        here = pl.ds(pl.multiple_of(low * piece + i * GROUP, GROUP), GROUP)
                        s = own[here, :] + mr[par, ks[0], inner, :].astype(F32) + mr[par, ks[1], inner, :].astype(F32)
                        s = (residual(here).astype(F32) + s).astype(BF)
                        bb[par, 0, pl.ds(pl.multiple_of(j * chunk + low * piece + i * GROUP, GROUP), GROUP), :] = store(here, s)

                    loop(piece // GROUP, some)

            @pl.when(v < units)
            def _():
                xr_copy(v).wait()

                def store(here, s):
                    hh[v, here, :] = s
                    return unit_norm(s.astype(F32), 1)

                finish(lambda here: xr[here, :], store)

            @pl.when(v >= units)
            def _():
                finish(lambda here: hh[v - units, here, :], lambda here, s: s)

            @pl.when(t >= 3)
            def _():
                for k in range(3):
                    pl.semaphore_wait(credit.at[k], 1)

            for k in range(4):
                g_copy(k, par).start()
            d_copy(0, par).start()

        @pl.when((t >= last) & (t < last + 2))
        def _():
            hand_on()

        @pl.when((t >= 2) & (t < last + 2))
        def _():
            for k in range(6):
                d_copy(k, old).wait_recv()

        @pl.when((t >= 2 + units) & (t < last + 2))
        def _():
            for k in range(2):
                y_copy(k, t - 2).start()

    def p3(t):
        par, old = lax.rem(t, 2), lax.rem(t + 1, 2)

        @pl.when((t >= 2 + units) & (t < last + 2))
        def _():
            for k in range(2):
                y_copy(k, t - 2).wait()

        @pl.when((t >= 2) & (t < last + 2))
        def _():
            for k in range(6):
                g_copy(k, par).wait_send()
                d_copy(k, par).wait_send()

        @pl.when((t >= 1) & (t <= last))
        def _():
            for k in (4, 5):
                m_copy(k, par).wait_send()

        @pl.when((t >= 0) & (t < last))
        def _():
            m_copy(0, par).wait_recv()
            stage(4, par, 1, 0, 0)
            m_copy(1, par).wait_recv()
            stage(5, par, -1, 1, 1)

            def keep(i):
                here = pl.ds(pl.multiple_of(j * chunk + i * GROUP, GROUP), GROUP)
                own[pl.ds(pl.multiple_of(i * GROUP, GROUP), GROUP), :] = part[here, :] + rr[par, here, :].astype(F32)

            loop(chunk // GROUP, keep)

        @pl.when((t >= 0) & (t < units))
        def _():
            xr_copy(t).start()

        @pl.when((t >= 1) & (t <= last))
        def _():
            for k in range(2):
                g_copy(k, old, came).wait_recv()
                g_copy(4 + k, old).start()
            for k in range(2):
                d_copy(1 + k, old).start()

    x_copy(0).start()
    for c in first_weights:
        c.start()
    tile_copy(wo, 0).start()
    for which, g in enumerate((ga, gm)):
        for n in range(d // LANE):
            gains[which : which + 1, n * LANE : (n + 1) * LANE] = g[n : n + 1, :].astype(F32)
    barrier = pltpu.get_barrier_semaphore()
    for peer in (left, right, twin):
        pl.semaphore_signal(barrier, inc=1, device_id={axis: peer}, device_id_type=pl.DeviceIdType.MESH)
    pl.semaphore_wait(barrier, 3)

    def period(i):
        t = i - 1
        p1(t)

        @pl.when(t < units - 2)
        def _():
            attend(t + 1)

        p2(t)

        @pl.when(t == units - 3)
        def _():
            attend(t + 2)
            gu_start(0, 0, WIDE)

        @pl.when((t >= 2) & (t < units + 2))
        def _():
            loop(full, lambda n: gate_up(t - 2, n, WIDE))

        p3(t)

        @pl.when(t < units - 1)
        def _():
            outward(t, lambda: seen[lax.rem(t + 1, 2)], wo)

        @pl.when((t >= units - 1) & (t < last - 1))
        def _():
            par = lax.rem(t - units + 1, 2)
            outward(t, lambda: hid[par], wd)

        if rest:
            @pl.when((t >= 2) & (t < units + 2))
            def _():
                gate_up(t - 2, full, rest)

    loop(last + 3, period)


def put_out(y, out, held, came, gone):
    per, n = held.shape[1], held.shape[0]
    rows = lambda ref, i: ref.at[i * per // ref.shape[1], pl.ds(i * per % ref.shape[1], per)]
    reads = [pltpu.make_async_copy(rows(y, i), held.at[i], came.at[i]) for i in range(n)]
    writes = [pltpu.make_async_copy(held.at[i], rows(out, i), gone.at[i]) for i in range(n)]
    for c in reads:
        c.start()
    for r, w in zip(reads, writes):
        r.wait()
        w.start()
    for w in writes:
        w.wait()


def solution(mesh):
    axis = "tp"
    chips = mesh.shape[axis] // 2

    def step(x, gain_a, wq, wk, wv, wo, gain_m, w_gate, w_up, w_down):
        units, rows, d = x.shape
        half, ff = rows // 2, w_gate.shape[1]
        chunk = half // chips
        qkv_width = wq.shape[1] + wk.shape[1] + wv.shape[1]
        buffer_width = max(qkv_width, 4 * WIDE)
        place = jnp.arange(rows)
        lane = jnp.arange(HEAD)
        angle = place.astype(F32)[:, None] * THETA ** (-(lane % (HEAD // 2)).astype(F32) / (HEAD // 2))
        cos, sin = jnp.cos(angle), jnp.where(lane < HEAD // 2, -1.0, 1.0) * jnp.sin(angle)
        hbm, vmem = pl.BlockSpec(memory_space=pl.ANY), pl.BlockSpec(memory_space=pltpu.VMEM)
        dma = lambda *shape: pltpu.SemaphoreType.DMA(shape)
        tiles = d // TILE
        y = pl.pallas_call(
            functools.partial(layer, axis, chips),
            out_shape=jax.ShapeDtypeStruct(x.shape, x.dtype),
            in_specs=[hbm, vmem, hbm, hbm, hbm, hbm, vmem, hbm, hbm, hbm, vmem, vmem],
            out_specs=hbm,
            scratch_shapes=[
                pltpu.VMEM((d, buffer_width), BF),
                pltpu.VMEM((max(ff, wo.shape[0]), 2 * TILE), BF),
                pltpu.VMEM((rows, d), BF),
                pltpu.VMEM((rows, qkv_width), BF),
                pltpu.VMEM((2, rows, wq.shape[1]), BF),
                pltpu.VMEM((2, rows, ff), BF),
                pltpu.VMEM((2, 2, half, d), BF),
                pltpu.VMEM((half, d), F32),
                pltpu.VMEM((half, d), BF),
                pltpu.VMEM((2, half, d), BF),
                pltpu.VMEM((6, chunk // 2, d), BF),
                pltpu.VMEM((2, 6, chunk // 2, d), BF),
                pltpu.VMEM((chunk, d), F32),
                pltpu.VMEM((chunk, d), BF),
                pltpu.VMEM((units, chunk, d), BF),
                pltpu.VMEM((2, d), F32),
                pltpu.SemaphoreType.DMA,
                dma(3, 2), dma(2), pltpu.SemaphoreType.DMA, dma(2),
                dma(tiles), dma(2, tiles), dma(6), dma(2, 6), dma(2, 6), dma(2, 6), dma(2, 6), dma(2, 6),
                pltpu.SemaphoreType.REGULAR((3,)),
            ],
            compiler_params=pltpu.CompilerParams(collective_id=0, has_side_effects=True, vmem_limit_bytes=67043328),
        )(x, gain_a.reshape(-1, LANE), wq, wk, wv, wo, gain_m.reshape(-1, LANE), w_gate, w_up, w_down, cos, sin)
        pieces, per = units * rows // 128, 128
        return pl.pallas_call(
            put_out,
            out_shape=jax.ShapeDtypeStruct(x.shape, x.dtype),
            in_specs=[hbm],
            out_specs=hbm,
            scratch_shapes=[pltpu.VMEM((pieces, per, d), BF), dma(pieces), dma(pieces)],
            compiler_params=pltpu.CompilerParams(vmem_limit_bytes=67043328),
        )(y)

    tokens, whole, columns, rows_of = P("dp", None, None), P(None), P(None, "tp"), P("tp", None)
    return jax.shard_map(
        step,
        mesh=mesh,
        in_specs=(tokens, whole, columns, columns, columns, rows_of, whole, columns, columns, rows_of),
        out_specs=tokens,
        check_vma=False,
    )
```

```python
import functools

import jax
import jax.numpy as jnp
from jax import lax
from jax.experimental import pallas as pl
from jax.experimental.pallas import tpu as pltpu
from jax.sharding import PartitionSpec as P

HEAD = 128
THETA = 10000
TILE = 512
LANE = 128
WIDE = 256
GROUP = 16
BF = jnp.bfloat16
F32 = jnp.float32


def layer(axis, chips, x, ga, wq, wk, wv, wo, gm, wg, wu, wd, cos, sin, y,
          wa, wt, xa, qkv, seen, hid, bb, part, sb, rr, st, mr, own, xr, hh, gains,
          x_sem, wa_sem, wt_sem, xr_sem, y_sem, r_send, r_recv, m_send, m_recv, g_send, g_recv, d_send, d_recv, credit):
    units, rows, d = x.shape
    last = 2 * units
    half = rows // 2
    chunk = half // chips
    piece = chunk // 2
    qw, kw = wq.shape[1], wk.shape[1]
    heads = qw // HEAD
    ff = wg.shape[1]
    full, rest = ff // WIDE, ff % WIDE
    blocks = full + (rest > 0)
    tiles = d // TILE
    me = lax.axis_index(axis)
    core, j = lax.rem(me, 2), lax.div(me, 2)
    chip = lambda by: lax.rem(j + by + chips, chips)
    left, right, twin = chip(-1) * 2 + core, chip(1) * 2 + core, j * 2 + 1 - core
    loop = lambda n, f: lax.fori_loop(0, n, lambda i, _: (f(i), None)[1], None)

    def remote(src, dst, send, recv, to):
        return pltpu.make_async_remote_copy(src_ref=src, dst_ref=dst, send_sem=send, recv_sem=recv, device_id={axis: to},
                                            device_id_type=pl.DeviceIdType.MESH)

    def m_copy(k, par):
        return remote(st.at[k], mr.at[par, k], m_send.at[k], m_recv.at[par, k], left if k % 2 else right)

    def at(by, low, n=piece):
        return pl.ds(pl.multiple_of(chip(by) * chunk + low * piece, piece), n)

    sent = ((0, 0), (0, 1), (0, 1), (0, 0), (-1, 0), (1, 1))
    came = ((-1, 0), (1, 1), (-1, 1), (1, 0), (2, 0), (2, 1))

    def g_copy(k, par, where=sent):
        ref = bb.at[par, 0, at(*where[k])]
        return remote(ref, ref, g_send.at[par, k], g_recv.at[par, k], left if k % 2 else right)

    handed = ((0, 0, chunk), (-1, 0), (1, 1), (-1, 1), (1, 0), (2, 0, chunk))

    def d_copy(k, par):
        here = at(*handed[k])
        return remote(bb.at[par, 0, here], bb.at[par, 1, here], d_send.at[par, k], d_recv.at[par, k], twin)

    def r_copy(n, par):
        cols = pl.ds(pl.multiple_of(n * TILE, TILE), TILE)
        return remote(sb.at[:, cols], rr.at[par, :, cols], r_send.at[n], r_recv.at[par, n], twin)

    def y_copy(k, v):
        par = lax.rem(v, 2)
        where = pl.ds(pl.multiple_of((core if k == 0 else 1 - core) * half, half), half)
        return pltpu.make_async_copy(bb.at[par, k], y.at[v - units, where], y_sem.at[k])

    def x_copy(u):
        return pltpu.make_async_copy(x.at[u], xa, x_sem)

    def xr_copy(u):
        where = pl.ds(pl.multiple_of(core * half + j * chunk, chunk), chunk)
        return pltpu.make_async_copy(x.at[u, where], xr, xr_sem)

    first_weights = [pltpu.make_async_copy(w, wa.at[:, a : a + w.shape[1]], wa_sem.at[n, 0])
                     for n, (w, a) in enumerate(((wq, 0), (wk, qw), (wv, qw + kw)))]

    def gu_slot(u, n, k, width):
        return pl.ds(pl.multiple_of(lax.rem(u * blocks + n, 2) * 2 * WIDE + k * width, LANE), width)

    def gu_copies(u, n, width):
        cols = pl.ds(pl.multiple_of(n * WIDE, WIDE), width)
        return [pltpu.make_async_copy(w.at[:, cols], wa.at[:, gu_slot(u, n, k, width)], wa_sem.at[lax.rem(u * blocks + n, 2), k])
                for k, w in enumerate((wg, wu))]

    def gu_start(u, n, width):
        for c in gu_copies(u, n, width):
            c.start()

    def tile_copy(w, n):
        cols = pl.ds(pl.multiple_of(n * TILE, TILE), TILE)
        slot = lax.rem(n, 2)
        return pltpu.make_async_copy(w.at[:, cols], wt.at[: w.shape[0], pl.ds(pl.multiple_of(slot * TILE, TILE), TILE)], wt_sem.at[slot])

    def unit_norm(wide, which):
        scale = lax.rsqrt(jnp.mean(wide * wide, -1, keepdims=True) + 1e-6)
        return (wide * scale * gains[which : which + 1, :]).astype(BF)

    def attend(u):
        x_copy(u).wait()

        def norm_rows(i):
            here = pl.ds(pl.multiple_of(i * GROUP, GROUP), GROUP)
            xa[here, :] = unit_norm(xa[here, :].astype(F32), 0)

        loop(rows // GROUP, norm_rows)

        @pl.when(u == 0)
        def _():
            for c in first_weights:
                c.wait()

        def project(i):
            here = pl.ds(pl.multiple_of(i * half, half), half)
            got = jnp.dot(xa[here, :], wa[:, : qw + 2 * kw], preferred_element_type=F32).astype(BF)
            c, s = cos[here, :], sin[here, :]
            for n in range(heads + 2):
                t = got[:, n * HEAD : (n + 1) * HEAD]
                if n < heads + 1:
                    w = t.astype(F32)
                    t = (w * c + pltpu.roll(w, HEAD // 2, 1) * s).astype(BF)
                qkv[here, n * HEAD : (n + 1) * HEAD] = t

        loop(2, project)

        @pl.when(u + 1 < units)
        def _():
            x_copy(u + 1).start()

        def head(n):
            cols = pl.ds(pl.multiple_of(n * HEAD, HEAD), HEAD)
            for i in range(2):
                keys = (i + 1) * half
                q, k, v = qkv[i * half : keys, cols], qkv[:keys, qw : qw + HEAD], qkv[:keys, qw + kw : qw + kw + HEAD]
                s = lax.dot_general(q, k, (((1,), (1,)), ((), ())), preferred_element_type=F32) * HEAD**-0.5
                ok = lax.broadcasted_iota(jnp.int32, s.shape, 0) + i * half >= lax.broadcasted_iota(jnp.int32, s.shape, 1)
                s = jnp.where(ok, s, -jnp.inf)
                e = jnp.exp(s - jnp.max(s, -1, keepdims=True))
                w = (e / jnp.sum(e, -1, keepdims=True)).astype(BF)
                to = pl.ds(pl.multiple_of((core if i == 0 else 1 - core) * half, half), half)
                seen[lax.rem(u, 2), to, cols] = jnp.dot(w, v, preferred_element_type=F32).astype(BF)

        loop(heads, head)

    def gate_up(u, n, width):
        par = lax.rem(u, 2)
        if width == WIDE:
            @pl.when(n + 1 < full)
            def _():
                gu_start(u, n + 1, WIDE)

            if rest:
                @pl.when(n + 1 == full)
                def _():
                    gu_start(u, n + 1, rest)

        if width == rest or not rest:
            @pl.when((n + 1 == blocks) & (u + 1 < units))
            def _():
                gu_start(u + 1, 0, WIDE)

        for c in gu_copies(u, n, width):
            c.wait()
        slot = pl.ds(pl.multiple_of(lax.rem(u * blocks + n, 2) * 2 * WIDE, 2 * WIDE), 2 * width)
        got = jnp.dot(bb[par].reshape(rows, d), wa[:, slot], preferred_element_type=F32)
        gate, up = got[:, :width], got[:, width:]
        hid[par, :, pl.ds(pl.multiple_of(n * WIDE, WIDE), width)] = (gate / (1 + jnp.exp(-gate)) * up).astype(BF)

    def outward(t, src, w):
        par = lax.rem(t + 1, 2)

        def one(n):
            @pl.when(n + 1 < tiles)
            def _():
                tile_copy(w, n + 1).start()

            tile_copy(w, n).wait()
            got = jnp.dot(src(), wt[: w.shape[0], pl.ds(pl.multiple_of(lax.rem(n, 2) * TILE, TILE), TILE)], preferred_element_type=F32)
            cols = pl.ds(pl.multiple_of(n * TILE, TILE), TILE)
            sb[:, cols] = got[half:].astype(BF)
            part[:, cols] = got[:half]
            r_copy(n, par).start()

        loop(tiles, one)

        @pl.when(t < units - 2)
        def _():
            tile_copy(wo, 0).start()

        @pl.when((t >= units - 2) & (t < last - 2))
        def _():
            tile_copy(wd, 0).start()

    def stage(k, par, by, low, extra=None):
        def some(i):
            here = pl.ds(pl.multiple_of(chip(by) * chunk + low * piece + i * GROUP, GROUP), GROUP)
            into = pl.ds(pl.multiple_of(i * GROUP, GROUP), GROUP)
            v = part[here, :] + rr[par, here, :].astype(F32)
            if extra is not None:
                v = v + mr[par, extra, into, :].astype(F32)
            st[k, into, :] = v.astype(BF)

        loop(piece // GROUP, some)
        m_copy(k, par).start()

    def p1(t):
        par = lax.rem(t, 2)

        @pl.when((t >= 1) & (t <= last))
        def _():
            for k in range(4):
                m_copy(k, par).wait_send()

        @pl.when((t >= 0) & (t < last))
        def _():
            def arrived(n):
                r_copy(n, par).wait_recv()
                r_copy(n, par).wait_send()

            loop(tiles, arrived)
            stage(0, par, 2, 0)
            stage(1, par, 2, 1)
            stage(2, par, 1, 1)
            stage(3, par, -1, 0)

    def hand_on(t):
        par = lax.rem(t, 2)
        for k in (2, 3):
            g_copy(k, par, came).wait_recv()
        for k in (3, 4):
            d_copy(k, par).start()
        for k in (4, 5):
            g_copy(k, par, came).wait_recv()
        d_copy(5, par).start()

    def p2(t):
        v = t - 1
        par, old = lax.rem(t + 1, 2), lax.rem(t, 2)

        @pl.when((t >= 3) & (t <= last))
        def _():
            for k, peer in enumerate((right, left, twin)):
                pl.semaphore_signal(credit.at[k], inc=1, device_id={axis: peer}, device_id_type=pl.DeviceIdType.MESH)

        @pl.when((t >= 1) & (t <= last))
        def _():
            for k in (2, 3, 4, 5):
                m_copy(k, par).wait_recv()

            def finish(residual, store):
                for low, ks in enumerate(((4, 3), (2, 5))):
                    def some(i):
                        inner = pl.ds(pl.multiple_of(i * GROUP, GROUP), GROUP)
                        here = pl.ds(pl.multiple_of(low * piece + i * GROUP, GROUP), GROUP)
                        s = own[here, :] + mr[par, ks[0], inner, :].astype(F32) + mr[par, ks[1], inner, :].astype(F32)
                        s = (residual(here).astype(F32) + s).astype(BF)
                        bb[par, 0, pl.ds(pl.multiple_of(j * chunk + low * piece + i * GROUP, GROUP), GROUP), :] = store(here, s)

                    loop(piece // GROUP, some)

            @pl.when(v < units)
            def _():
                xr_copy(v).wait()

                def store(here, s):
                    hh[v, here, :] = s
                    return unit_norm(s.astype(F32), 1)

                finish(lambda here: xr[here, :], store)

            @pl.when(v >= units)
            def _():
                finish(lambda here: hh[v - units, here, :], lambda here, s: s)

            @pl.when(t >= 3)
            def _():
                for k in range(3):
                    pl.semaphore_wait(credit.at[k], 1)

            for k in range(4):
                g_copy(k, par).start()
            d_copy(0, par).start()

        @pl.when((t >= last) & (t < last + 2))
        def _():
            hand_on(t)

        @pl.when((t >= 2) & (t < last + 2))
        def _():
            for k in range(6):
                d_copy(k, old).wait_recv()

        @pl.when((t >= 2 + units) & (t < last + 2))
        def _():
            for k in range(2):
                y_copy(k, t - 2).start()

    def p3(t):
        par, old = lax.rem(t, 2), lax.rem(t + 1, 2)

        @pl.when((t >= 2 + units) & (t < last + 2))
        def _():
            for k in range(2):
                y_copy(k, t - 2).wait()

        @pl.when((t >= 2) & (t < last + 2))
        def _():
            for k in range(6):
                g_copy(k, par).wait_send()
                d_copy(k, par).wait_send()

        @pl.when((t >= 1) & (t <= last))
        def _():
            for k in (4, 5):
                m_copy(k, par).wait_send()

        @pl.when((t >= 0) & (t < last))
        def _():
            m_copy(0, par).wait_recv()
            stage(4, par, 1, 0, 0)
            m_copy(1, par).wait_recv()
            stage(5, par, -1, 1, 1)

            def keep(i):
                here = pl.ds(pl.multiple_of(j * chunk + i * GROUP, GROUP), GROUP)
                own[pl.ds(pl.multiple_of(i * GROUP, GROUP), GROUP), :] = part[here, :] + rr[par, here, :].astype(F32)

            loop(chunk // GROUP, keep)

        @pl.when((t >= 0) & (t < units))
        def _():
            xr_copy(t).start()

        @pl.when((t >= 1) & (t <= last))
        def _():
            for k in range(2):
                g_copy(k, old, came).wait_recv()
                g_copy(4 + k, old).start()
            for k in range(2):
                d_copy(1 + k, old).start()

    x_copy(0).start()
    for c in first_weights:
        c.start()
    tile_copy(wo, 0).start()
    for which, g in enumerate((ga, gm)):
        for n in range(d // LANE):
            gains[which : which + 1, n * LANE : (n + 1) * LANE] = g[n : n + 1, :].astype(F32)
    barrier = pltpu.get_barrier_semaphore()
    for peer in (left, right, twin):
        pl.semaphore_signal(barrier, inc=1, device_id={axis: peer}, device_id_type=pl.DeviceIdType.MESH)
    pl.semaphore_wait(barrier, 3)

    def period(i):
        t = i - 1
        p1(t)

        @pl.when(t < units - 2)
        def _():
            attend(t + 1)

        after = (t >= 3) & (t < units + 3)

        @pl.when(after)
        def _():
            first = full - 1 - (t - 3)
            loop(full - first, lambda n: gate_up(t - 3, first + n, WIDE))

        @pl.when((t >= 2) & (t < last))
        def _():
            hand_on(t)

        if rest:
            @pl.when(after)
            def _():
                gate_up(t - 3, full, rest)

        p2(t)

        @pl.when(t == units - 3)
        def _():
            attend(t + 2)
            gu_start(0, 0, WIDE)

        @pl.when((t >= 2) & (t < units + 2))
        def _():
            loop(full - 1 - (t - 2), lambda n: gate_up(t - 2, n, WIDE))

        p3(t)

        @pl.when(t < units - 1)
        def _():
            outward(t, lambda: seen[lax.rem(t + 1, 2)], wo)

        @pl.when((t >= units - 1) & (t < last - 1))
        def _():
            par = lax.rem(t - units + 1, 2)
            outward(t, lambda: hid[par], wd)

    loop(last + 3, period)


def put_out(y, out, held, came, gone):
    per, n = held.shape[1], held.shape[0]
    rows = lambda ref, i: ref.at[i * per // ref.shape[1], pl.ds(i * per % ref.shape[1], per)]
    reads = [pltpu.make_async_copy(rows(y, i), held.at[i], came.at[i]) for i in range(n)]
    writes = [pltpu.make_async_copy(held.at[i], rows(out, i), gone.at[i]) for i in range(n)]
    for c in reads:
        c.start()
    for r, w in zip(reads, writes):
        r.wait()
        w.start()
    for w in writes:
        w.wait()


def solution(mesh):
    axis = "tp"
    chips = mesh.shape[axis] // 2

    def step(x, gain_a, wq, wk, wv, wo, gain_m, w_gate, w_up, w_down):
        units, rows, d = x.shape
        half, ff = rows // 2, w_gate.shape[1]
        chunk = half // chips
        qkv_width = wq.shape[1] + wk.shape[1] + wv.shape[1]
        buffer_width = max(qkv_width, 4 * WIDE)
        place = jnp.arange(rows)
        lane = jnp.arange(HEAD)
        angle = place.astype(F32)[:, None] * THETA ** (-(lane % (HEAD // 2)).astype(F32) / (HEAD // 2))
        cos, sin = jnp.cos(angle), jnp.where(lane < HEAD // 2, -1.0, 1.0) * jnp.sin(angle)
        hbm, vmem = pl.BlockSpec(memory_space=pl.ANY), pl.BlockSpec(memory_space=pltpu.VMEM)
        dma = lambda *shape: pltpu.SemaphoreType.DMA(shape)
        tiles = d // TILE
        y = pl.pallas_call(
            functools.partial(layer, axis, chips),
            out_shape=jax.ShapeDtypeStruct(x.shape, x.dtype),
            in_specs=[hbm, vmem, hbm, hbm, hbm, hbm, vmem, hbm, hbm, hbm, vmem, vmem],
            out_specs=hbm,
            scratch_shapes=[
                pltpu.VMEM((d, buffer_width), BF),
                pltpu.VMEM((max(ff, wo.shape[0]), 2 * TILE), BF),
                pltpu.VMEM((rows, d), BF),
                pltpu.VMEM((rows, qkv_width), BF),
                pltpu.VMEM((2, rows, wq.shape[1]), BF),
                pltpu.VMEM((2, rows, ff), BF),
                pltpu.VMEM((2, 2, half, d), BF),
                pltpu.VMEM((half, d), F32),
                pltpu.VMEM((half, d), BF),
                pltpu.VMEM((2, half, d), BF),
                pltpu.VMEM((6, chunk // 2, d), BF),
                pltpu.VMEM((2, 6, chunk // 2, d), BF),
                pltpu.VMEM((chunk, d), F32),
                pltpu.VMEM((chunk, d), BF),
                pltpu.VMEM((units, chunk, d), BF),
                pltpu.VMEM((2, d), F32),
                pltpu.SemaphoreType.DMA,
                dma(3, 2), dma(2), pltpu.SemaphoreType.DMA, dma(2),
                dma(tiles), dma(2, tiles), dma(6), dma(2, 6), dma(2, 6), dma(2, 6), dma(2, 6), dma(2, 6),
                pltpu.SemaphoreType.REGULAR((3,)),
            ],
            compiler_params=pltpu.CompilerParams(collective_id=0, has_side_effects=True, vmem_limit_bytes=67043328),
        )(x, gain_a.reshape(-1, LANE), wq, wk, wv, wo, gain_m.reshape(-1, LANE), w_gate, w_up, w_down, cos, sin)
        pieces, per = units * rows // 128, 128
        return pl.pallas_call(
            put_out,
            out_shape=jax.ShapeDtypeStruct(x.shape, x.dtype),
            in_specs=[hbm],
            out_specs=hbm,
            scratch_shapes=[pltpu.VMEM((pieces, per, d), BF), dma(pieces), dma(pieces)],
            compiler_params=pltpu.CompilerParams(vmem_limit_bytes=67043328),
        )(y)

    tokens, whole, columns, rows_of = P("dp", None, None), P(None), P(None, "tp"), P("tp", None)
    return jax.shard_map(
        step,
        mesh=mesh,
        in_specs=(tokens, whole, columns, columns, columns, rows_of, whole, columns, columns, rows_of),
        out_specs=tokens,
        check_vma=False,
    )
```

```python
import functools

import jax
import jax.numpy as jnp
import numpy as np
from jax import lax
from jax.experimental import pallas as pl
from jax.experimental.pallas import tpu as pltpu
from jax.sharding import PartitionSpec as P

HEAD = 128
THETA = 10000
TILE = 512
LANE = 128
WIDE = 256
GROUP = 16
BF = jnp.bfloat16
F32 = jnp.float32


def layer(axis, chips, x, ga, wq, wk, wv, wo, gm, wg, wu, wd, cos, sin, y,
          wa, wt, xa, qkv, seen, hid, bb, part, sb, rr, st, mr, own, xr, hh, gains,
          x_sem, wa_sem, wt_sem, xr_sem, y_sem, r_send, r_recv, m_send, m_recv, g_send, g_recv, d_send, d_recv, credit):
    units, rows, d = x.shape
    last = 2 * units
    half = rows // 2
    chunk = half // chips
    piece = chunk // 2
    qw, kw = wq.shape[1], wk.shape[1]
    heads = qw // HEAD
    ff = wg.shape[1]
    full, rest = ff // WIDE, ff % WIDE
    blocks = full + (rest > 0)
    tiles = d // TILE
    me = lax.axis_index(axis)
    core, j = lax.rem(me, 2), lax.div(me, 2)
    chip = lambda by: lax.rem(j + by + chips, chips)
    left, right, twin = chip(-1) * 2 + core, chip(1) * 2 + core, j * 2 + 1 - core
    loop = lambda n, f: lax.fori_loop(0, n, lambda i, _: (f(i), None)[1], None)

    def remote(src, dst, send, recv, to):
        return pltpu.make_async_remote_copy(src_ref=src, dst_ref=dst, send_sem=send, recv_sem=recv, device_id={axis: to},
                                            device_id_type=pl.DeviceIdType.MESH)

    def m_copy(k, par):
        some = pl.ds(2 * k, 2) if k < 2 else pl.ds(k + 2, 1)
        return remote(st.at[some], mr.at[par, some], m_send.at[k], m_recv.at[par, k], left if k % 2 else right)

    def at(by, low, n=piece):
        return pl.ds(pl.multiple_of(chip(by) * chunk + low * piece, piece), n)

    sent = ((0, 0), (0, 1), (0, 1), (0, 0), (-1, 0), (1, 1))
    came = ((-1, 0), (1, 1), (-1, 1), (1, 0), (2, 0), (2, 1))

    def g_copy(k, par, where=sent):
        ref = bb.at[par, 0, at(*where[k])]
        return remote(ref, ref, g_send.at[par, k], g_recv.at[par, k], left if k % 2 else right)

    handed = ((0, 0, chunk), (-1, 0), (1, 1), (-1, 1), (1, 0), (2, 0, chunk))

    def d_copy(k, par):
        here = at(*handed[k])
        return remote(bb.at[par, 0, here], bb.at[par, 1, here], d_send.at[par, k], d_recv.at[par, k], twin)

    def r_copy(n, par):
        cols = pl.ds(pl.multiple_of(n * TILE, TILE), TILE)
        return remote(sb.at[:, cols], rr.at[par, :, cols], r_send.at[n], r_recv.at[par, n], twin)

    def y_copy(k, v):
        par, by = lax.rem(v, 2), (0, -1, 1, 2)[k % 4]
        where = pl.ds(pl.multiple_of((core if k < 4 else 1 - core) * half + chip(by) * chunk, chunk), chunk)
        return pltpu.make_async_copy(bb.at[par, k // 4, at(by, 0, chunk)], y.at[v - units, where], y_sem.at[k])

    def y_start(t, ks):
        @pl.when(t >= 2 + units)
        def _():
            for k in ks:
                y_copy(k, t - 2).start()

    def x_copy(u, k):
        here = pl.ds(pl.multiple_of(k * half, half), half)
        return pltpu.make_async_copy(x.at[u, here], xa.at[here], x_sem.at[k])

    def x_start(u):
        for k in range(2):
            x_copy(u, k).start()

    def xr_copy(u):
        where = pl.ds(pl.multiple_of(core * half + j * chunk, chunk), chunk)
        return pltpu.make_async_copy(x.at[u, where], xr, xr_sem)

    first_weights = [pltpu.make_async_copy(w, wa.at[:, a : a + w.shape[1]], wa_sem.at[n, 0])
                     for n, (w, a) in enumerate(((wq, 0), (wk, qw), (wv, qw + kw)))]

    def gu_slot(u, n, k, width):
        return pl.ds(pl.multiple_of(lax.rem(u * blocks + n, 2) * 2 * WIDE + k * width, LANE), width)

    def gu_copies(u, n, width):
        cols = pl.ds(pl.multiple_of(n * WIDE, WIDE), width)
        return [pltpu.make_async_copy(w.at[:, cols], wa.at[:, gu_slot(u, n, k, width)], wa_sem.at[lax.rem(u * blocks + n, 2), k])
                for k, w in enumerate((wg, wu))]

    def gu_start(u, n, width):
        for c in gu_copies(u, n, width):
            c.start()

    def tile_copy(w, n):
        cols = pl.ds(pl.multiple_of(n * TILE, TILE), TILE)
        slot = lax.rem(n, 2)
        return pltpu.make_async_copy(w.at[:, cols], wt.at[: w.shape[0], pl.ds(pl.multiple_of(slot * TILE, TILE), TILE)], wt_sem.at[slot])

    def unit_norm(wide, which):
        scale = lax.rsqrt(jnp.mean(wide * wide, -1, keepdims=True) + 1e-6)
        return (wide * scale * gains[which : which + 1, :]).astype(BF)

    def attend(u):
        def norm_rows(i):
            for k in range(2):
                @pl.when(i == k * (half // GROUP))
                def _():
                    x_copy(u, k).wait()

            here = pl.ds(pl.multiple_of(i * GROUP, GROUP), GROUP)
            xa[here, :] = unit_norm(xa[here, :].astype(F32), 0)

        loop(rows // GROUP, norm_rows)

        @pl.when(u == 0)
        def _():
            for c in first_weights:
                c.wait()

        def project(i):
            here = pl.ds(pl.multiple_of(i * half, half), half)
            got = jnp.dot(xa[here, :], wa[:, : qw + 2 * kw], preferred_element_type=F32).astype(BF)
            c, s = cos[here, :], sin[here, :]
            for n in range(heads + 2):
                t = got[:, n * HEAD : (n + 1) * HEAD]
                if n < heads + 1:
                    w = t.astype(F32)
                    t = (w * c + pltpu.roll(w, HEAD // 2, 1) * s).astype(BF)
                qkv[here, n * HEAD : (n + 1) * HEAD] = t

        loop(2, project)

        @pl.when(u + 1 < units)
        def _():
            x_start(u + 1)

        def head(n):
            cols = pl.ds(pl.multiple_of(n * HEAD, HEAD), HEAD)
            for i in range(2):
                keys = (i + 1) * half
                q, k, v = qkv[i * half : keys, cols], qkv[:keys, qw : qw + HEAD], qkv[:keys, qw + kw : qw + kw + HEAD]
                s = lax.dot_general(q, k, (((1,), (1,)), ((), ())), preferred_element_type=F32) * HEAD**-0.5
                ok = lax.broadcasted_iota(jnp.int32, s.shape, 0) + i * half >= lax.broadcasted_iota(jnp.int32, s.shape, 1)
                s = jnp.where(ok, s, -jnp.inf)
                e = jnp.exp(s - jnp.max(s, -1, keepdims=True))
                w = (e / jnp.sum(e, -1, keepdims=True)).astype(BF)
                to = pl.ds(pl.multiple_of((core if i == 0 else 1 - core) * half, half), half)
                seen[lax.rem(u, 2), to, cols] = jnp.dot(w, v, preferred_element_type=F32).astype(BF)

        loop(heads, head)

    def gate_up(u, n, width):
        par = lax.rem(u, 2)
        if width == WIDE:
            @pl.when(n + 1 < full)
            def _():
                gu_start(u, n + 1, WIDE)

            if rest:
                @pl.when(n + 1 == full)
                def _():
                    gu_start(u, n + 1, rest)

        if width == rest or not rest:
            @pl.when((n + 1 == blocks) & (u + 1 < units))
            def _():
                gu_start(u + 1, 0, WIDE)

        for c in gu_copies(u, n, width):
            c.wait()
        slot = pl.ds(pl.multiple_of(lax.rem(u * blocks + n, 2) * 2 * WIDE, 2 * WIDE), 2 * width)
        got = jnp.dot(bb[par].reshape(rows, d), wa[:, slot], preferred_element_type=F32)
        gate, up = got[:, :width], got[:, width:]
        hid[par, :, pl.ds(pl.multiple_of(n * WIDE, WIDE), width)] = (gate / (1 + jnp.exp(-gate)) * up).astype(BF)

    def outward(t, src, w):
        par = lax.rem(t + 1, 2)

        def one(n):
            @pl.when(n + 1 < tiles)
            def _():
                tile_copy(w, n + 1).start()

            tile_copy(w, n).wait()
            got = jnp.dot(src(), wt[: w.shape[0], pl.ds(pl.multiple_of(lax.rem(n, 2) * TILE, TILE), TILE)], preferred_element_type=F32)
            cols = pl.ds(pl.multiple_of(n * TILE, TILE), TILE)
            sb[:, cols] = got[half:].astype(BF)
            part[:, cols] = got[:half]
            r_copy(n, par).start()

        loop(tiles, one)

        @pl.when(t < units - 2)
        def _():
            tile_copy(wo, 0).start()

        @pl.when((t >= units - 2) & (t < last - 2))
        def _():
            tile_copy(wd, 0).start()

    def stage(k, par, by, low, extra=None):
        def some(i):
            here = pl.ds(pl.multiple_of(chip(by) * chunk + low * piece + i * GROUP, GROUP), GROUP)
            into = pl.ds(pl.multiple_of(i * GROUP, GROUP), GROUP)
            v = part[here, :] + rr[par, here, :].astype(F32)
            if extra is not None:
                v = v + mr[par, extra, into, :].astype(F32)
            st[k, into, :] = v.astype(BF)

        loop(piece // GROUP, some)

    def p1(t):
        par = lax.rem(t, 2)

        @pl.when((t >= 1) & (t <= last))
        def _():
            for k in range(2):
                m_copy(k, par).wait_send()

        @pl.when((t >= 0) & (t < last))
        def _():
            def arrived(n):
                r_copy(n, par).wait_recv()
                r_copy(n, par).wait_send()

            loop(tiles, arrived)
            stage(0, par, 2, 0)
            stage(1, par, 1, 1)
            m_copy(0, par).start()
            stage(2, par, 2, 1)
            stage(3, par, -1, 0)
            m_copy(1, par).start()

    def hand_on(t):
        par = lax.rem(t, 2)
        for k in (2, 3):
            g_copy(k, par, came).wait_recv()
        for k in (3, 4):
            d_copy(k, par).start()
        y_start(t, (0, 1, 2))
        for k in (4, 5):
            g_copy(k, par, came).wait_recv()
        d_copy(5, par).start()
        y_start(t, (3,))

    def p2(t):
        v = t - 1
        par, old = lax.rem(t + 1, 2), lax.rem(t, 2)

        @pl.when((t >= 3) & (t <= last))
        def _():
            for k, peer in enumerate((right, left, twin)):
                pl.semaphore_signal(credit.at[k], inc=1, device_id={axis: peer}, device_id_type=pl.DeviceIdType.MESH)

        @pl.when((t >= 1) & (t <= last))
        def _():
            for k in (2, 3):
                m_copy(k, par).wait_recv()

            def finish(residual, store):
                for low, ks in enumerate(((4, 3), (1, 5))):
                    def some(i):
                        inner = pl.ds(pl.multiple_of(i * GROUP, GROUP), GROUP)
                        here = pl.ds(pl.multiple_of(low * piece + i * GROUP, GROUP), GROUP)
                        s = own[here, :] + mr[par, ks[0], inner, :].astype(F32) + mr[par, ks[1], inner, :].astype(F32)
                        s = (residual(here).astype(F32) + s).astype(BF)
                        bb[par, 0, pl.ds(pl.multiple_of(j * chunk + low * piece + i * GROUP, GROUP), GROUP), :] = store(here, s)

                    loop(piece // GROUP, some)

            @pl.when(v < units)
            def _():
                xr_copy(v).wait()

                def store(here, s):
                    hh[v, here, :] = s
                    return unit_norm(s.astype(F32), 1)

                finish(lambda here: xr[here, :], store)

            @pl.when(v >= units)
            def _():
                finish(lambda here: hh[v - units, here, :], lambda here, s: s)

            @pl.when(t >= 3)
            def _():
                for k in range(3):
                    pl.semaphore_wait(credit.at[k], 1)

            for k in range(4):
                g_copy(k, par).start()
            d_copy(0, par).start()

        @pl.when((t >= last) & (t < last + 2))
        def _():
            hand_on(t)

        @pl.when((t >= 2) & (t < last + 2))
        def _():
            for k in range(5):
                d_copy(k, old).wait_recv()
            y_start(t, (4, 5, 6))
            d_copy(5, old).wait_recv()
            y_start(t, (7,))

    def p3(t):
        par, old = lax.rem(t, 2), lax.rem(t + 1, 2)

        @pl.when((t >= 2 + units) & (t < last + 2))
        def _():
            for k in range(8):
                y_copy(k, t - 2).wait()

        @pl.when((t >= 2) & (t < last + 2))
        def _():
            for k in range(6):
                g_copy(k, par).wait_send()
                d_copy(k, par).wait_send()

        @pl.when((t >= 1) & (t <= last))
        def _():
            for k in (2, 3):
                m_copy(k, par).wait_send()

        @pl.when((t >= 0) & (t < last))
        def _():
            m_copy(0, par).wait_recv()
            stage(4, par, 1, 0, 0)
            m_copy(2, par).start()
            m_copy(1, par).wait_recv()
            stage(5, par, -1, 1, 2)
            m_copy(3, par).start()

            def keep(i):
                here = pl.ds(pl.multiple_of(j * chunk + i * GROUP, GROUP), GROUP)
                own[pl.ds(pl.multiple_of(i * GROUP, GROUP), GROUP), :] = part[here, :] + rr[par, here, :].astype(F32)

            loop(chunk // GROUP, keep)

        @pl.when((t >= 0) & (t < units))
        def _():
            xr_copy(t).start()

        @pl.when((t >= 1) & (t <= last))
        def _():
            for k in range(2):
                g_copy(k, old, came).wait_recv()
                g_copy(4 + k, old).start()
            for k in range(2):
                d_copy(1 + k, old).start()

    x_start(0)
    for c in first_weights:
        c.start()
    tile_copy(wo, 0).start()
    for which, g in enumerate((ga, gm)):
        for n in range(d // LANE):
            gains[which : which + 1, n * LANE : (n + 1) * LANE] = g[n : n + 1, :].astype(F32)
    barrier = pltpu.get_barrier_semaphore()
    for peer in (left, right, twin):
        pl.semaphore_signal(barrier, inc=1, device_id={axis: peer}, device_id_type=pl.DeviceIdType.MESH)
    pl.semaphore_wait(barrier, 3)

    def period(i):
        t = i - 1
        p1(t)

        @pl.when(t < units - 2)
        def _():
            attend(t + 1)

        after = (t >= 3) & (t < units + 3)

        @pl.when(after)
        def _():
            first = full - 1 - (t - 3)
            loop(full - first, lambda n: gate_up(t - 3, first + n, WIDE))

        @pl.when((t >= 2) & (t < last))
        def _():
            hand_on(t)

        if rest:
            @pl.when(after)
            def _():
                gate_up(t - 3, full, rest)

        p2(t)

        @pl.when(t == units - 3)
        def _():
            attend(t + 2)
            gu_start(0, 0, WIDE)

        @pl.when((t >= 2) & (t < units + 2))
        def _():
            loop(full - 1 - (t - 2), lambda n: gate_up(t - 2, n, WIDE))

        p3(t)

        @pl.when(t < units - 1)
        def _():
            outward(t, lambda: seen[lax.rem(t + 1, 2)], wo)

        @pl.when((t >= units - 1) & (t < last - 1))
        def _():
            par = lax.rem(t - units + 1, 2)
            outward(t, lambda: hid[par], wd)

    loop(last + 3, period)


def put_out(y, out, held, came, gone):
    per, n = held.shape[1], held.shape[0]
    rows = lambda ref, i: ref.at[i * per // ref.shape[1], pl.ds(i * per % ref.shape[1], per)]
    reads = [pltpu.make_async_copy(rows(y, i), held.at[i], came.at[i]) for i in range(n)]
    writes = [pltpu.make_async_copy(held.at[i], rows(out, i), gone.at[i]) for i in range(n)]
    for c in reads:
        c.start()
    for r, w in zip(reads, writes):
        r.wait()
        w.start()
    for w in writes:
        w.wait()


def solution(mesh):
    axis = "tp"
    chips = mesh.shape[axis] // 2

    def step(x, gain_a, wq, wk, wv, wo, gain_m, w_gate, w_up, w_down):
        units, rows, d = x.shape
        half, ff = rows // 2, w_gate.shape[1]
        chunk = half // chips
        qkv_width = wq.shape[1] + wk.shape[1] + wv.shape[1]
        buffer_width = max(qkv_width, 4 * WIDE)
        lane = np.arange(HEAD)
        turn = np.float32(THETA) ** (-(lane % (HEAD // 2)).astype(np.float32) / np.float32(HEAD // 2))
        angle = np.arange(rows, dtype=np.float32)[:, None] * turn
        cos = jnp.asarray(np.cos(angle), F32)
        sin = jnp.asarray(np.where(lane < HEAD // 2, -1, 1) * np.sin(angle), F32)
        hbm, vmem = pl.BlockSpec(memory_space=pl.ANY), pl.BlockSpec(memory_space=pltpu.VMEM)
        dma = lambda *shape: pltpu.SemaphoreType.DMA(shape)
        tiles = d // TILE
        y = pl.pallas_call(
            functools.partial(layer, axis, chips),
            out_shape=jax.ShapeDtypeStruct(x.shape, x.dtype),
            in_specs=[hbm, vmem, hbm, hbm, hbm, hbm, vmem, hbm, hbm, hbm, vmem, vmem],
            out_specs=hbm,
            scratch_shapes=[
                pltpu.VMEM((d, buffer_width), BF),
                pltpu.VMEM((max(ff, wo.shape[0]), 2 * TILE), BF),
                pltpu.VMEM((rows, d), BF),
                pltpu.VMEM((rows, qkv_width), BF),
                pltpu.VMEM((2, rows, wq.shape[1]), BF),
                pltpu.VMEM((2, rows, ff), BF),
                pltpu.VMEM((2, 2, half, d), BF),
                pltpu.VMEM((half, d), F32),
                pltpu.VMEM((half, d), BF),
                pltpu.VMEM((2, half, d), BF),
                pltpu.VMEM((6, chunk // 2, d), BF),
                pltpu.VMEM((2, 6, chunk // 2, d), BF),
                pltpu.VMEM((chunk, d), F32),
                pltpu.VMEM((chunk, d), BF),
                pltpu.VMEM((units, chunk, d), BF),
                pltpu.VMEM((2, d), F32),
                dma(2), dma(3, 2), dma(2), pltpu.SemaphoreType.DMA, dma(8),
                dma(tiles), dma(2, tiles), dma(4), dma(2, 4), dma(2, 6), dma(2, 6), dma(2, 6), dma(2, 6),
                pltpu.SemaphoreType.REGULAR((3,)),
            ],
            compiler_params=pltpu.CompilerParams(collective_id=0, has_side_effects=True, vmem_limit_bytes=67043328),
        )(x, gain_a.reshape(-1, LANE), wq, wk, wv, wo, gain_m.reshape(-1, LANE), w_gate, w_up, w_down, cos, sin)
        pieces, per = units * rows // 128, 128
        return pl.pallas_call(
            put_out,
            out_shape=jax.ShapeDtypeStruct(x.shape, x.dtype),
            in_specs=[hbm],
            out_specs=hbm,
            scratch_shapes=[pltpu.VMEM((pieces, per, d), BF), dma(pieces), dma(pieces)],
            compiler_params=pltpu.CompilerParams(vmem_limit_bytes=67043328),
        )(y)

    tokens, whole, columns, rows_of = P("dp", None, None), P(None), P(None, "tp"), P("tp", None)
    return jax.shard_map(
        step,
        mesh=mesh,
        in_specs=(tokens, whole, columns, columns, columns, rows_of, whole, columns, columns, rows_of),
        out_specs=tokens,
        check_vma=False,
    )
```

```python
import functools

import jax
import jax.numpy as jnp
import numpy as np
from jax import lax
from jax.experimental import pallas as pl
from jax.experimental.pallas import tpu as pltpu
from jax.sharding import PartitionSpec as P

HEAD = 128
THETA = 10000
AHEAD = 2
TILE = 512
LANE = 128
WIDE = 256
GROUP = 16
BF = jnp.bfloat16
F32 = jnp.float32


def layer(axis, chips, x, ga, wq, wk, wv, wo, gm, wg, wu, wd, cos, sin, y,
          wa, wt, xa, qkv, seen, hid, bb, part, sb, rr, st, mr, own, xr, hh, gains,
          x_sem, wa_sem, wt_sem, xr_sem, y_sem, r_send, r_recv, m_send, m_recv, g_send, g_recv, d_send, d_recv, credit):
    units, rows, d = x.shape
    last = 2 * units
    half = rows // 2
    chunk = half // chips
    piece = chunk // 2
    qw, kw = wq.shape[1], wk.shape[1]
    heads = qw // HEAD
    ff = wg.shape[1]
    full, rest = ff // WIDE, ff % WIDE
    blocks = full + (rest > 0)
    tiles = d // TILE
    me = lax.axis_index(axis)
    core, j = lax.rem(me, 2), lax.div(me, 2)
    chip = lambda by: lax.rem(j + by + chips, chips)
    left, right, twin = chip(-1) * 2 + core, chip(1) * 2 + core, j * 2 + 1 - core
    loop = lambda n, f: lax.fori_loop(0, n, lambda i, _: (f(i), None)[1], None)

    def remote(src, dst, send, recv, to):
        return pltpu.make_async_remote_copy(src_ref=src, dst_ref=dst, send_sem=send, recv_sem=recv, device_id={axis: to},
                                            device_id_type=pl.DeviceIdType.MESH)

    def m_copy(k, par):
        some = pl.ds(2 * k, 2) if k < 2 else pl.ds(k + 2, 1)
        return remote(st.at[some], mr.at[par, some], m_send.at[k], m_recv.at[par, k], left if k % 2 else right)

    def at(by, low, n=piece):
        return pl.ds(pl.multiple_of(chip(by) * chunk + low * piece, piece), n)

    sent = ((0, 0), (0, 1), (0, 1), (0, 0), (-1, 0), (1, 1))
    came = ((-1, 0), (1, 1), (-1, 1), (1, 0), (2, 0), (2, 1))

    def g_copy(k, par, where=sent):
        ref = bb.at[par, 0, at(*where[k])]
        return remote(ref, ref, g_send.at[par, k], g_recv.at[par, k], left if k % 2 else right)

    handed = ((0, 0, chunk), (-1, 0), (1, 1), (-1, 1), (1, 0), (2, 0, chunk))

    def d_copy(k, par):
        here = at(*handed[k])
        return remote(bb.at[par, 0, here], bb.at[par, 1, here], d_send.at[par, k], d_recv.at[par, k], twin)

    def r_copy(n, par):
        cols = pl.ds(pl.multiple_of(n * TILE, TILE), TILE)
        return remote(sb.at[:, cols], rr.at[par, :, cols], r_send.at[n], r_recv.at[par, n], twin)

    def y_copy(k, v):
        par, by = lax.rem(v, 2), (0, -1, 1, 2)[k % 4]
        where = pl.ds(pl.multiple_of((core if k < 4 else 1 - core) * half + chip(by) * chunk, chunk), chunk)
        return pltpu.make_async_copy(bb.at[par, k // 4, at(by, 0, chunk)], y.at[v - units, where], y_sem.at[k])

    def y_start(t, ks):
        @pl.when(t >= 2 + units)
        def _():
            for k in ks:
                y_copy(k, t - 2).start()

    def x_copy(u, k):
        here = pl.ds(pl.multiple_of(k * half, half), half)
        return pltpu.make_async_copy(x.at[u, here], xa.at[here], x_sem.at[k])

    def x_start(u):
        for k in range(2):
            x_copy(u, k).start()

    def xr_copy(u):
        where = pl.ds(pl.multiple_of(core * half + j * chunk, chunk), chunk)
        return pltpu.make_async_copy(x.at[u, where], xr, xr_sem)

    first_weights = [pltpu.make_async_copy(w, wa.at[:, a : a + w.shape[1]], wa_sem.at[n, 0])
                     for n, (w, a) in enumerate(((wq, 0), (wk, qw), (wv, qw + kw)))]

    def gu_slot(u, n, k, width):
        return pl.ds(pl.multiple_of(lax.rem(u * blocks + n, 2) * 2 * WIDE + k * width, LANE), width)

    def gu_copies(u, n, width):
        cols = pl.ds(pl.multiple_of(n * WIDE, WIDE), width)
        return [pltpu.make_async_copy(w.at[:, cols], wa.at[:, gu_slot(u, n, k, width)], wa_sem.at[lax.rem(u * blocks + n, 2), k])
                for k, w in enumerate((wg, wu))]

    def gu_start(u, n, width):
        for c in gu_copies(u, n, width):
            c.start()

    def tile_copy(w, t, n):
        cols = pl.ds(pl.multiple_of(n * TILE, TILE), TILE)
        slot = lax.rem((t + 1) * tiles + n, AHEAD + 1)
        return pltpu.make_async_copy(w.at[:, cols], wt.at[: w.shape[0], pl.ds(pl.multiple_of(slot * TILE, TILE), TILE)], wt_sem.at[slot])

    def unit_norm(wide, which):
        scale = lax.rsqrt(jnp.mean(wide * wide, -1, keepdims=True) + 1e-6)
        return (wide * scale * gains[which : which + 1, :]).astype(BF)

    def attend(u):
        def norm_rows(i):
            for k in range(2):
                @pl.when(i == k * (half // GROUP))
                def _():
                    x_copy(u, k).wait()

            here = pl.ds(pl.multiple_of(i * GROUP, GROUP), GROUP)
            xa[here, :] = unit_norm(xa[here, :].astype(F32), 0)

        loop(rows // GROUP, norm_rows)

        @pl.when(u == 0)
        def _():
            for c in first_weights:
                c.wait()

        def project(i):
            here = pl.ds(pl.multiple_of(i * half, half), half)
            got = jnp.dot(xa[here, :], wa[:, : qw + 2 * kw], preferred_element_type=F32).astype(BF)
            c, s = cos[here, :], sin[here, :]
            for n in range(heads + 2):
                t = got[:, n * HEAD : (n + 1) * HEAD]
                if n < heads + 1:
                    w = t.astype(F32)
                    t = (w * c + pltpu.roll(w, HEAD // 2, 1) * s).astype(BF)
                qkv[here, n * HEAD : (n + 1) * HEAD] = t

        loop(2, project)

        @pl.when(u + 1 < units)
        def _():
            x_start(u + 1)

        def head(n):
            cols = pl.ds(pl.multiple_of(n * HEAD, HEAD), HEAD)
            for i in range(2):
                keys = (i + 1) * half
                q, k, v = qkv[i * half : keys, cols], qkv[:keys, qw : qw + HEAD], qkv[:keys, qw + kw : qw + kw + HEAD]
                s = lax.dot_general(q, k, (((1,), (1,)), ((), ())), preferred_element_type=F32) * HEAD**-0.5
                ok = lax.broadcasted_iota(jnp.int32, s.shape, 0) + i * half >= lax.broadcasted_iota(jnp.int32, s.shape, 1)
                s = jnp.where(ok, s, -jnp.inf)
                e = jnp.exp(s - jnp.max(s, -1, keepdims=True))
                w = (e / jnp.sum(e, -1, keepdims=True)).astype(BF)
                to = pl.ds(pl.multiple_of((core if i == 0 else 1 - core) * half, half), half)
                seen[lax.rem(u, 2), to, cols] = jnp.dot(w, v, preferred_element_type=F32).astype(BF)

        loop(heads, head)

    def gate_up(u, n, width):
        par = lax.rem(u, 2)
        if width == WIDE:
            @pl.when(n + 1 < full)
            def _():
                gu_start(u, n + 1, WIDE)

            if rest:
                @pl.when(n + 1 == full)
                def _():
                    gu_start(u, n + 1, rest)

        if width == rest or not rest:
            @pl.when((n + 1 == blocks) & (u + 1 < units))
            def _():
                gu_start(u + 1, 0, WIDE)

        for c in gu_copies(u, n, width):
            c.wait()
        slot = pl.ds(pl.multiple_of(lax.rem(u * blocks + n, 2) * 2 * WIDE, 2 * WIDE), 2 * width)
        got = jnp.dot(bb[par].reshape(rows, d), wa[:, slot], preferred_element_type=F32)
        gate, up = got[:, :width], got[:, width:]
        hid[par, :, pl.ds(pl.multiple_of(n * WIDE, WIDE), width)] = (gate / (1 + jnp.exp(-gate)) * up).astype(BF)

    def outward(t, src, w):
        par = lax.rem(t + 1, 2)

        def one(n):
            later = n + AHEAD

            @pl.when(later < tiles)
            def _():
                tile_copy(w, t, later).start()

            @pl.when((later >= tiles) & (t < units - 2))
            def _():
                tile_copy(wo, t + 1, later - tiles).start()

            @pl.when((later >= tiles) & (t >= units - 2) & (t < last - 2))
            def _():
                tile_copy(wd, t + 1, later - tiles).start()

            tile_copy(w, t, n).wait()
            got = jnp.dot(src(), wt[: w.shape[0], pl.ds(pl.multiple_of(lax.rem((t + 1) * tiles + n, AHEAD + 1) * TILE, TILE), TILE)], preferred_element_type=F32)
            cols = pl.ds(pl.multiple_of(n * TILE, TILE), TILE)
            sb[:, cols] = got[half:].astype(BF)
            part[:, cols] = got[:half]
            r_copy(n, par).start()

        loop(tiles, one)

    def stage(k, par, by, low, extra=None):
        def some(i):
            here = pl.ds(pl.multiple_of(chip(by) * chunk + low * piece + i * GROUP, GROUP), GROUP)
            into = pl.ds(pl.multiple_of(i * GROUP, GROUP), GROUP)
            v = part[here, :] + rr[par, here, :].astype(F32)
            if extra is not None:
                v = v + mr[par, extra, into, :].astype(F32)
            st[k, into, :] = v.astype(BF)

        loop(piece // GROUP, some)

    def p1(t):
        par = lax.rem(t, 2)

        @pl.when((t >= 1) & (t <= last))
        def _():
            for k in range(2):
                m_copy(k, par).wait_send()

        @pl.when((t >= 0) & (t < last))
        def _():
            def arrived(n):
                r_copy(n, par).wait_recv()
                r_copy(n, par).wait_send()

            loop(tiles, arrived)
            stage(0, par, 2, 0)
            stage(1, par, 1, 1)
            m_copy(0, par).start()
            stage(2, par, 2, 1)
            stage(3, par, -1, 0)
            m_copy(1, par).start()

    def hand_on(t):
        par = lax.rem(t, 2)
        for k in (2, 3):
            g_copy(k, par, came).wait_recv()
        for k in (3, 4):
            d_copy(k, par).start()
        y_start(t, (0, 1, 2))
        for k in (4, 5):
            g_copy(k, par, came).wait_recv()
        d_copy(5, par).start()
        y_start(t, (3,))

    def p2(t):
        v = t - 1
        par, old = lax.rem(t + 1, 2), lax.rem(t, 2)

        @pl.when((t >= 3) & (t <= last))
        def _():
            for k, peer in enumerate((right, left, twin)):
                pl.semaphore_signal(credit.at[k], inc=1, device_id={axis: peer}, device_id_type=pl.DeviceIdType.MESH)

        @pl.when((t >= 1) & (t <= last))
        def _():
            for k in (2, 3):
                m_copy(k, par).wait_recv()

            def finish(residual, store):
                for low, ks in enumerate(((4, 3), (1, 5))):
                    def some(i):
                        inner = pl.ds(pl.multiple_of(i * GROUP, GROUP), GROUP)
                        here = pl.ds(pl.multiple_of(low * piece + i * GROUP, GROUP), GROUP)
                        s = own[here, :] + mr[par, ks[0], inner, :].astype(F32) + mr[par, ks[1], inner, :].astype(F32)
                        s = (residual(here).astype(F32) + s).astype(BF)
                        bb[par, 0, pl.ds(pl.multiple_of(j * chunk + low * piece + i * GROUP, GROUP), GROUP), :] = store(here, s)

                    loop(piece // GROUP, some)

            @pl.when(v < units)
            def _():
                xr_copy(v).wait()

                def store(here, s):
                    hh[v, here, :] = s
                    return unit_norm(s.astype(F32), 1)

                finish(lambda here: xr[here, :], store)

            @pl.when(v >= units)
            def _():
                finish(lambda here: hh[v - units, here, :], lambda here, s: s)

            @pl.when(t >= 3)
            def _():
                for k in range(3):
                    pl.semaphore_wait(credit.at[k], 1)

            for k in range(4):
                g_copy(k, par).start()
            d_copy(0, par).start()

        @pl.when((t >= last) & (t < last + 2))
        def _():
            hand_on(t)

        @pl.when((t >= 2) & (t < last + 2))
        def _():
            for k in range(5):
                d_copy(k, old).wait_recv()
            y_start(t, (4, 5, 6))
            d_copy(5, old).wait_recv()
            y_start(t, (7,))

    def p3(t):
        par, old = lax.rem(t, 2), lax.rem(t + 1, 2)

        @pl.when((t >= 2 + units) & (t < last + 2))
        def _():
            for k in range(8):
                y_copy(k, t - 2).wait()

        @pl.when((t >= 2) & (t < last + 2))
        def _():
            for k in range(6):
                g_copy(k, par).wait_send()
                d_copy(k, par).wait_send()

        @pl.when((t >= 1) & (t <= last))
        def _():
            for k in (2, 3):
                m_copy(k, par).wait_send()

        @pl.when((t >= 0) & (t < last))
        def _():
            m_copy(0, par).wait_recv()
            stage(4, par, 1, 0, 0)
            m_copy(2, par).start()
            m_copy(1, par).wait_recv()
            stage(5, par, -1, 1, 2)
            m_copy(3, par).start()

            def keep(i):
                here = pl.ds(pl.multiple_of(j * chunk + i * GROUP, GROUP), GROUP)
                own[pl.ds(pl.multiple_of(i * GROUP, GROUP), GROUP), :] = part[here, :] + rr[par, here, :].astype(F32)

            loop(chunk // GROUP, keep)

        @pl.when((t >= 0) & (t < units))
        def _():
            xr_copy(t).start()

        @pl.when((t >= 1) & (t <= last))
        def _():
            for k in range(2):
                g_copy(k, old, came).wait_recv()
                g_copy(4 + k, old).start()
            for k in range(2):
                d_copy(1 + k, old).start()

    x_start(0)
    for c in first_weights:
        c.start()
    for n in range(AHEAD):
        tile_copy(wo, jnp.int32(-1), jnp.int32(n)).start()
    for which, g in enumerate((ga, gm)):
        for n in range(d // LANE):
            gains[which : which + 1, n * LANE : (n + 1) * LANE] = g[n : n + 1, :].astype(F32)
    barrier = pltpu.get_barrier_semaphore()
    for peer in (left, right, twin):
        pl.semaphore_signal(barrier, inc=1, device_id={axis: peer}, device_id_type=pl.DeviceIdType.MESH)
    pl.semaphore_wait(barrier, 3)

    def period(i):
        t = i - 1
        p1(t)

        @pl.when(t < units - 2)
        def _():
            attend(t + 1)

        after = (t >= 3) & (t < units + 3)

        @pl.when(after)
        def _():
            first = full - 1 - (t - 3)
            loop(full - first, lambda n: gate_up(t - 3, first + n, WIDE))

        @pl.when((t >= 2) & (t < last))
        def _():
            hand_on(t)

        if rest:
            @pl.when(after)
            def _():
                gate_up(t - 3, full, rest)

        p2(t)

        @pl.when(t == units - 3)
        def _():
            attend(t + 2)
            gu_start(0, 0, WIDE)

        @pl.when((t >= 2) & (t < units + 2))
        def _():
            loop(full - 1 - (t - 2), lambda n: gate_up(t - 2, n, WIDE))

        p3(t)

        @pl.when(t < units - 1)
        def _():
            outward(t, lambda: seen[lax.rem(t + 1, 2)], wo)

        @pl.when((t >= units - 1) & (t < last - 1))
        def _():
            par = lax.rem(t - units + 1, 2)
            outward(t, lambda: hid[par], wd)

    loop(last + 3, period)


def put_out(y, out, held, came, gone):
    per, n = held.shape[1], held.shape[0]
    rows = lambda ref, i: ref.at[i * per // ref.shape[1], pl.ds(i * per % ref.shape[1], per)]
    reads = [pltpu.make_async_copy(rows(y, i), held.at[i], came.at[i]) for i in range(n)]
    writes = [pltpu.make_async_copy(held.at[i], rows(out, i), gone.at[i]) for i in range(n)]
    for c in reads:
        c.start()
    for r, w in zip(reads, writes):
        r.wait()
        w.start()
    for w in writes:
        w.wait()


def solution(mesh):
    axis = "tp"
    chips = mesh.shape[axis] // 2

    def step(x, gain_a, wq, wk, wv, wo, gain_m, w_gate, w_up, w_down):
        units, rows, d = x.shape
        half, ff = rows // 2, w_gate.shape[1]
        chunk = half // chips
        qkv_width = wq.shape[1] + wk.shape[1] + wv.shape[1]
        buffer_width = max(qkv_width, 4 * WIDE)
        lane = np.arange(HEAD)
        turn = np.float32(THETA) ** (-(lane % (HEAD // 2)).astype(np.float32) / np.float32(HEAD // 2))
        angle = np.arange(rows, dtype=np.float32)[:, None] * turn
        cos = jnp.asarray(np.cos(angle), F32)
        sin = jnp.asarray(np.where(lane < HEAD // 2, -1, 1) * np.sin(angle), F32)
        hbm, vmem = pl.BlockSpec(memory_space=pl.ANY), pl.BlockSpec(memory_space=pltpu.VMEM)
        dma = lambda *shape: pltpu.SemaphoreType.DMA(shape)
        tiles = d // TILE
        y = pl.pallas_call(
            functools.partial(layer, axis, chips),
            out_shape=jax.ShapeDtypeStruct(x.shape, x.dtype),
            in_specs=[hbm, vmem, hbm, hbm, hbm, hbm, vmem, hbm, hbm, hbm, vmem, vmem],
            out_specs=hbm,
            scratch_shapes=[
                pltpu.VMEM((d, buffer_width), BF),
                pltpu.VMEM((max(ff, wo.shape[0]), (AHEAD + 1) * TILE), BF),
                pltpu.VMEM((rows, d), BF),
                pltpu.VMEM((rows, qkv_width), BF),
                pltpu.VMEM((2, rows, wq.shape[1]), BF),
                pltpu.VMEM((2, rows, ff), BF),
                pltpu.VMEM((2, 2, half, d), BF),
                pltpu.VMEM((half, d), F32),
                pltpu.VMEM((half, d), BF),
                pltpu.VMEM((2, half, d), BF),
                pltpu.VMEM((6, chunk // 2, d), BF),
                pltpu.VMEM((2, 6, chunk // 2, d), BF),
                pltpu.VMEM((chunk, d), F32),
                pltpu.VMEM((chunk, d), BF),
                pltpu.VMEM((units, chunk, d), BF),
                pltpu.VMEM((2, d), F32),
                dma(2), dma(3, 2), dma(AHEAD + 1), pltpu.SemaphoreType.DMA, dma(8),
                dma(tiles), dma(2, tiles), dma(4), dma(2, 4), dma(2, 6), dma(2, 6), dma(2, 6), dma(2, 6),
                pltpu.SemaphoreType.REGULAR((3,)),
            ],
            compiler_params=pltpu.CompilerParams(collective_id=0, has_side_effects=True, vmem_limit_bytes=67043328),
        )(x, gain_a.reshape(-1, LANE), wq, wk, wv, wo, gain_m.reshape(-1, LANE), w_gate, w_up, w_down, cos, sin)
        pieces, per = units * rows // 128, 128
        return pl.pallas_call(
            put_out,
            out_shape=jax.ShapeDtypeStruct(x.shape, x.dtype),
            in_specs=[hbm],
            out_specs=hbm,
            scratch_shapes=[pltpu.VMEM((pieces, per, d), BF), dma(pieces), dma(pieces)],
            compiler_params=pltpu.CompilerParams(vmem_limit_bytes=67043328),
        )(y)

    tokens, whole, columns, rows_of = P("dp", None, None), P(None), P(None, "tp"), P("tp", None)
    return jax.shard_map(
        step,
        mesh=mesh,
        in_specs=(tokens, whole, columns, columns, columns, rows_of, whole, columns, columns, rows_of),
        out_specs=tokens,
        check_vma=False,
    )
```
